32 devices in a mesh: ctx: 4 (over y, core), exp: 8 (over z, x).
Axes of the slice: x: 2, y: 2, z: 4, core: 2. Of those that a mesh axis runs over, the one named last changes fastest.
Arguments:
- queries: bfloat16 [512, 64, 576], P('ctx', 'exp'), may hold values from -1024 to 1024
- latents: bfloat16 [512, 576], P('ctx'), may hold values from -6.1 to 6.1
- block_starts: int32 [8], replicated, may hold values from 0 to 448, as said below
- w_uv: bfloat16 [64, 512, 128], P('exp'), may hold values from -0.25 to 0.25
- moe_tokens: bfloat16 [1024, 7168], P('exp'), may hold values from -6 to 6
- expert_ids: int32 [1024, 2], P('exp'), may hold values from 0 to 7, as said below
- gate_weights: float32 [1024, 2], P('exp'), may hold values from 0.2 to 1
- w_gate: bfloat16 [8, 7168, 512], P('exp', None, 'ctx'), may hold values from -0.0625 to 0.0625
- w_up: bfloat16 [8, 7168, 512], P('exp', None, 'ctx'), may hold values from -0.0625 to 0.0625
- w_down: bfloat16 [8, 512, 7168], P('exp', 'ctx'), may hold values from -0.25 to 0.25
Outputs:
- attended: bfloat16 [512, 64, 128], P('ctx', 'exp')
- moe_out: bfloat16 [1024, 7168], P('exp', 'ctx')
The draws below stay inside these ranges and needn't reach their ends.
Inputs may be any that keep to these rules, and one draw needn't show every extreme that they name: Token t has position block_starts[t // 64] + t % 64; block_starts is a permutation of the multiples of 64 below 512. `expert_ids`: each row names 2 different experts. In the rows of one index of exp, one expert, the same for every index, is named by exactly 48 rows, no expert by more, and the other experts' counts differ by at most one.
All inputs are finite; a program needn't handle non-finite values.
Results may differ from the reference program's by a relative error of at most 0.018.
Values may be sent and summed in bfloat16 or wider, within the bound.
No kernel may reach another device: no remote copies, remote signals or barrier semaphores. Data moves between devices by JAX's collectives and lax.ppermute only.
A program may use at most 128 MiB of HBM per device.

```python
import math
import jax
import jax.numpy as jnp
from jax import lax

D = 7168
LAT = 512
ROPE = 64
VDIM = 128
F_DEV = 128
S_DEV = 128
MT_DEV = 128
TOP = 2
HEADS = 64
FF = 512
TOKENS_A = 512
MT_TOK = 1024
EXPERTS = 8
CAP = 48
N_CTX = 4
N_EXP = 8


def block_order(key):
    return jax.random.permutation(jax.random.fold_in(key, 11), 2 * TOKENS_A // S_DEV).astype(jnp.int32)


def draw_block_starts(key, part):
    return (block_order(key) * (S_DEV // 2)).astype(jnp.int32)


def base_latents(key):
    drawn = jax.random.normal(jax.random.fold_in(key, 12), (TOKENS_A, LAT + ROPE), jnp.float32)
    return jnp.clip(drawn, -6.0, 6.0)


def draw_latents(key, part):
    base = base_latents(key)
    return base.astype(jnp.bfloat16)


def draw_queries(key, part):
    base = jax.random.normal(jax.random.fold_in(key, 13), (TOKENS_A, HEADS, LAT + ROPE), jnp.float32)
    base = jnp.clip(base, -6.0, 6.0)
    return base.astype(jnp.bfloat16)


def draw_expert_ids(key, part):
    full = jax.random.randint(jax.random.fold_in(key, 21), (), 0, EXPERTS)
    column = jnp.arange(TOP, dtype=jnp.int32)[None, :]

    def one_block(block_index):
        inner = jax.random.fold_in(key, 100 + block_index)
        ranking = jax.random.permutation(jax.random.fold_in(inner, 1), MT_DEV).astype(jnp.int32)[:, None]
        offset = jax.random.randint(jax.random.fold_in(inner, 2), (), 0, EXPERTS - 1)
        leading = ranking < CAP
        sequence = jnp.where(leading, ranking * (TOP - 1) + column - 1, CAP * (TOP - 1) + (ranking - CAP) * TOP + column)
        others = (sequence + offset) % (EXPERTS - 1)
        others = others + (others >= full).astype(jnp.int32)
        return jnp.where(leading & (column == 0), full, others).astype(jnp.int32)
    blocks = jax.vmap(one_block)(jnp.arange(MT_TOK // MT_DEV, dtype=jnp.int32))
    return blocks.reshape(MT_TOK, TOP).astype(jnp.int32)


def levels(stream_key, extent, shards, least, high):
    def one(axis_at, parts):
        draws = jax.random.uniform(jax.random.fold_in(jax.random.fold_in(stream_key, 6), axis_at), (parts,), jnp.float32, least / len(shards), high / len(shards))
        return jnp.repeat(jnp.exp(draws), extent[axis_at] // parts).reshape((-1,) + (1,) * (len(extent) - axis_at - 1))

    factor_of = one(*shards[0])
    for cut in shards[1:]:
        factor_of = factor_of * one(*cut)
    return factor_of


def noise(key, dims, spread, reach, split=(), held_as=jnp.bfloat16):
    level = levels(key, dims, split, -0.22, 0.18) if split else 1.0
    entries = jax.random.normal(key, dims, jnp.float32) * spread * level
    return jnp.minimum(jnp.maximum(entries, -reach), reach).astype(held_as)


def setup_inputs(seed: int = 0) -> dict:
    splits = jax.random.split(jax.random.key(seed), 11)
    return {
        "queries": draw_queries(jax.random.fold_in(splits[10], 71), 0),
        "latents": draw_latents(jax.random.fold_in(splits[10], 71), 0),
        "block_starts": draw_block_starts(jax.random.fold_in(splits[10], 71), 0),
        "w_uv": noise(splits[3], (HEADS, LAT, VDIM), LAT ** -0.5, 0.25, ((0, 8),)),
        "moe_tokens": noise(splits[4], (MT_TOK, D), 1.0, 6.0, ((0, 8),)),
        "expert_ids": draw_expert_ids(jax.random.fold_in(splits[10], 71), 0),
        "gate_weights": jnp.clip(0.2 + 0.8 * jax.random.uniform(splits[6], (MT_TOK, TOP), jnp.float32) ** levels(splits[6], (MT_TOK, TOP), ((0, 8),), -0.2, 0.2), 0.2, 1.0),
        "w_gate": noise(splits[7], (EXPERTS, D, FF), D ** -0.5, 0.0625, ((0, 8), (2, 4))),
        "w_up": noise(splits[8], (EXPERTS, D, FF), D ** -0.5, 0.0625, ((0, 8), (2, 4))),
        "w_down": noise(splits[9], (EXPERTS, FF, D), FF ** -0.5, 0.25, ((0, 8), (1, 4))),
    }


score_scale = (0.1 * math.log(40.0) + 1.0) ** 2 / math.sqrt(192.0)
neg_fill = -1e+30

def token_positions(block_starts, token_index, half_block):
    block_index = token_index // half_block
    matches = block_index[:, None] == jnp.arange(block_starts.shape[0], dtype=jnp.int32)[None, :]
    first_pos = lax.optimization_barrier(jnp.sum(jnp.where(matches, block_starts[None, :], 0), axis=1))
    return (first_pos + token_index % half_block).astype(jnp.int32)

def slot_targets(expert_ids, expert_count, capacity):
    token_count, picks = expert_ids.shape
    flat_ids = expert_ids.reshape(token_count * picks)
    onehot = (flat_ids[:, None] == jnp.arange(expert_count, dtype=jnp.int32)[None, :]).astype(jnp.int32)
    earlier = jnp.cumsum(onehot, axis=0) - onehot
    slot_index = lax.optimization_barrier(jnp.sum(earlier * onehot, axis=1))
    return (flat_ids * capacity + slot_index).astype(jnp.int32)

def reference(queries, latents, block_starts, w_uv, moe_tokens, expert_ids, gate_weights, w_gate, w_up, w_down):
    positions = token_positions(block_starts, jnp.arange(TOKENS_A, dtype=jnp.int32), S_DEV // 2)
    visible = positions[None, :] <= positions[:, None]
    values = latents[:, :LAT]

    def one_head(pieces):
        head_queries, head_uv = pieces
        scores = jnp.dot(head_queries, latents.T, preferred_element_type=jnp.float32) * score_scale
        masked = jnp.where(visible, scores, neg_fill)
        top_score = lax.optimization_barrier(jnp.max(masked, axis=1, keepdims=True))
        weights = jnp.where(visible, jnp.exp(masked - top_score), 0.0)
        totals = lax.optimization_barrier(jnp.sum(weights, axis=1, keepdims=True))
        blended = jnp.dot(weights.astype(jnp.bfloat16), values, preferred_element_type=jnp.float32)
        latent_out = (blended / totals).astype(jnp.bfloat16)
        return jnp.dot(latent_out, head_uv, preferred_element_type=jnp.float32).astype(jnp.bfloat16)
    per_head = lax.map(one_head, (jnp.transpose(queries, (1, 0, 2)), w_uv))
    attended = jnp.transpose(per_head, (1, 0, 2))
    block_ids = expert_ids.reshape(N_EXP, MT_DEV, TOP)
    targets = jax.vmap(lambda ids: slot_targets(ids, EXPERTS, CAP))(block_ids)
    local_rows = jnp.arange(MT_DEV * TOP, dtype=jnp.int32) // TOP
    global_rows = jnp.arange(N_EXP, dtype=jnp.int32)[:, None] * MT_DEV + local_rows[None, :]

    def fill_block(target_row, token_row, gate_row):
        filled = jnp.zeros((EXPERTS * CAP,), jnp.int32).at[target_row].set(token_row + 1)
        scaled = jnp.zeros((EXPERTS * CAP,), jnp.float32).at[target_row].set(gate_row)
        return (filled, scaled)
    filled, scaled = jax.vmap(fill_block)(targets, global_rows, gate_weights.reshape(N_EXP, MT_DEV * TOP))
    filled = jnp.transpose(filled.reshape(N_EXP, EXPERTS, CAP), (1, 0, 2)).reshape(EXPERTS, N_EXP * CAP)
    scaled = jnp.transpose(scaled.reshape(N_EXP, EXPERTS, CAP), (1, 0, 2)).reshape(EXPERTS, N_EXP * CAP)

    def one_expert(accum, pieces):
        slot_rows, slot_gates, gate_matrix, up_matrix, down_matrix = pieces
        occupied = slot_rows > 0
        source = jnp.where(occupied, slot_rows - 1, 0)
        inputs = jnp.where(occupied[:, None], moe_tokens[source], 0)
        gate_h = jnp.dot(inputs, gate_matrix, preferred_element_type=jnp.float32)
        up_h = jnp.dot(inputs, up_matrix, preferred_element_type=jnp.float32)
        hidden = (jax.nn.silu(gate_h) * up_h).astype(jnp.bfloat16)

        def add_group(group_index, summed):
            begin = (group_index * F_DEV).astype(jnp.int32)
            hidden_part = lax.dynamic_slice_in_dim(hidden, begin, F_DEV, 1)
            down_part = lax.dynamic_slice_in_dim(down_matrix, begin, F_DEV, 0)
            rounded = jnp.dot(hidden_part, down_part, preferred_element_type=jnp.float32).astype(jnp.bfloat16)
            return summed + lax.optimization_barrier(rounded).astype(jnp.float32)
        summed = lax.fori_loop(0, N_CTX, add_group, jnp.zeros((N_EXP * CAP, D), jnp.float32))
        contrib = jnp.where(occupied[:, None], slot_gates[:, None] * summed, 0.0)
        return (accum.at[source].add(contrib), None)
    accum, _ = lax.scan(one_expert, jnp.zeros((MT_TOK, D), jnp.float32), (filled, scaled, w_gate, w_up, w_down))
    return (attended, accum.astype(jnp.bfloat16))
```

```python
import functools
import math

import jax
import jax.numpy as jnp
from jax import lax
from jax.experimental import pallas as pl
from jax.experimental.pallas import tpu as pltpu
from jax.sharding import PartitionSpec as P

score_scale = (0.1 * math.log(40.0) + 1.0) ** 2 / math.sqrt(192.0)
neg_fill = -1e30


def swap(x, axis, offset):
    size = lax.axis_size(axis)
    return lax.ppermute(x, axis, [(i, i ^ offset) for i in range(size)])


def gather_xor(x, axis="ctx"):
    size = lax.axis_size(axis)
    even = [x] + [swap(x, axis, offset) for offset in range(2, size, 2)]
    joined = jnp.stack(even)
    other = swap(joined, axis, 1)
    blocks = []
    for i in range(len(even)):
        blocks += [even[i], other[i]]
    return blocks


def token_positions(block_starts, token_index, half_block):
    block_index = token_index // half_block
    matches = block_index[:, None] == jnp.arange(block_starts.shape[0], dtype=jnp.int32)[None, :]
    first_pos = jnp.sum(jnp.where(matches, block_starts[None, :], 0), axis=1)
    return first_pos + token_index % half_block


def slot_ranks(ids, expert_count):
    token_count = ids.shape[1]
    experts = lax.broadcasted_iota(jnp.int32, (expert_count, token_count), 0)
    named = jnp.zeros((expert_count, token_count), jnp.float32)
    for k in range(ids.shape[0]):
        named = named + jnp.where(ids[k : k + 1, :] == experts, 1.0, 0.0)
    rows = lax.broadcasted_iota(jnp.int32, (token_count, token_count), 0)
    cols = lax.broadcasted_iota(jnp.int32, (token_count, token_count), 1)
    before = jnp.where(rows < cols, 1.0, 0.0).astype(jnp.bfloat16)
    rank = jnp.dot(named.astype(jnp.bfloat16), before, preferred_element_type=jnp.float32)
    return named, rank


def dispatch_kernel(capacity, me_ref, ids_ref, tokens_ref, *refs):
    out_refs, named_ref, rank_ref = refs[:-2], refs[-2], refs[-1]
    expert_count = len(out_refs)
    token_count = ids_ref.shape[1]
    named, rank = slot_ranks(ids_ref[...], expert_count)
    named_ref[...] = named
    rank_ref[...] = rank
    tokens = tokens_ref[...]
    slots = lax.broadcasted_iota(jnp.int32, (capacity, token_count), 0).astype(jnp.float32)
    for k in range(expert_count):
        expert = me_ref[0] ^ k
        row_named = named_ref[pl.ds(expert, 1), :]
        row_rank = rank_ref[pl.ds(expert, 1), :]
        pick = jnp.where((row_rank == slots) & (row_named > 0.5), 1.0, 0.0).astype(jnp.bfloat16)
        rows = jnp.dot(pick, tokens, preferred_element_type=jnp.float32)
        out_refs[k][...] = rows.astype(out_refs[k].dtype)


def dispatch(tokens, ids, capacity, expert_count):
    token_count, model_width = tokens.shape
    width = model_width // lax.axis_size("ctx")
    me, mine = lax.axis_index("exp").astype(jnp.int32), lax.axis_index("ctx").astype(jnp.int32)
    if width % 128:
        tokens = lax.dynamic_slice_in_dim(tokens, mine * width, width, axis=1)
        mine = jnp.zeros_like(mine)
    where = jnp.stack([me, mine])
    return pl.pallas_call(
        functools.partial(dispatch_kernel, capacity),
        out_shape=[jax.ShapeDtypeStruct((capacity, width), tokens.dtype)] * expert_count,
        grid_spec=pltpu.PrefetchScalarGridSpec(
            num_scalar_prefetch=1,
            grid=(1,),
            in_specs=[
                pl.BlockSpec(ids.shape, lambda i, w: (0, 0)),
                pl.BlockSpec((token_count, width), lambda i, w: (0, w[1])),
            ],
            out_specs=[pl.BlockSpec((capacity, width), lambda i, w: (0, 0))] * expert_count,
            scratch_shapes=[
                pltpu.VMEM((expert_count, token_count), jnp.float32),
                pltpu.VMEM((expert_count, token_count), jnp.float32),
            ],
        ),
        cost_estimate=pl.CostEstimate(
            flops=2 * expert_count * capacity * token_count * width,
            bytes_accessed=2 * width * (token_count + expert_count * capacity),
            transcendentals=0,
        ),
        name="dispatch",
    )(where, ids, tokens)


def combine_kernel(capacity, me_ref, ids_ref, gates_ref, *refs):
    row_refs, out_ref, named_ref, rank_ref = refs[:-3], refs[-3], refs[-2], refs[-1]
    expert_count = len(row_refs)
    picks, token_count = ids_ref.shape
    ids = ids_ref[...]
    named, rank = slot_ranks(ids, expert_count)
    named_ref[...] = named
    rank_ref[...] = rank
    slots = lax.broadcasted_iota(jnp.int32, (capacity, token_count), 0).astype(jnp.float32)
    sums = [None] * picks
    for k in range(expert_count):
        expert = me_ref[0] ^ k
        row_rank = rank_ref[pl.ds(expert, 1), :]
        rows = row_refs[k][...]
        for j in range(picks):
            chosen = ids[j : j + 1, :] == expert
            pick = jnp.where((row_rank == slots) & chosen, 1.0, 0.0).astype(jnp.bfloat16)
            part = lax.dot_general(
                pick, rows, (((0,), (0,)), ((), ())), preferred_element_type=jnp.float32
            )
            sums[j] = part if sums[j] is None else sums[j] + part
    gates = gates_ref[...]
    total = sums[0] * gates[:, 0:1]
    for j in range(1, picks):
        total = total + sums[j] * gates[:, j : j + 1]
    out_ref[...] = total.astype(out_ref.dtype)


def combine(row_blocks, ids, gates):
    capacity, width = row_blocks[0].shape
    picks, token_count = ids.shape
    expert_count = len(row_blocks)
    where = lax.axis_index("exp").astype(jnp.int32).reshape(1)
    steps = 1 if width % 256 else 2
    part = width // steps
    return pl.pallas_call(
        functools.partial(combine_kernel, capacity),
        out_shape=jax.ShapeDtypeStruct((token_count, width), row_blocks[0].dtype),
        grid_spec=pltpu.PrefetchScalarGridSpec(
            num_scalar_prefetch=1,
            grid=(steps,),
            in_specs=[
                pl.BlockSpec(ids.shape, lambda i, w: (0, 0)),
                pl.BlockSpec(gates.shape, lambda i, w: (0, 0)),
            ]
            + [pl.BlockSpec((capacity, part), lambda i, w: (0, i))] * expert_count,
            out_specs=pl.BlockSpec((token_count, part), lambda i, w: (0, i)),
            scratch_shapes=[
                pltpu.VMEM((expert_count, token_count), jnp.float32),
                pltpu.VMEM((expert_count, token_count), jnp.float32),
            ],
        ),
        cost_estimate=pl.CostEstimate(
            flops=2 * picks * expert_count * capacity * token_count * width,
            bytes_accessed=2 * width * (token_count + expert_count * capacity),
            transcendentals=0,
        ),
        name="combine",
    )(where, ids, gates, *row_blocks)


def attention(queries, latents, block_starts, w_uv):
    query_tokens, head_count, entry_width = queries.shape
    lat_width = w_uv.shape[1]
    half_block = query_tokens // 2
    row_total = query_tokens * head_count
    mine = lax.axis_index("ctx")
    ctx_size = lax.axis_size("ctx")
    offsets = jnp.arange(query_tokens, dtype=jnp.int32)
    own_positions = token_positions(block_starts, mine * query_tokens + offsets, half_block)
    query_positions = jnp.repeat(own_positions, head_count)
    keys = jnp.concatenate(gather_xor(latents), axis=0)
    owners = jnp.bitwise_xor(mine.astype(jnp.int32), jnp.arange(ctx_size, dtype=jnp.int32))
    key_index = (owners[:, None] * query_tokens + offsets[None, :]).reshape(-1)
    key_positions = token_positions(block_starts, key_index, half_block)
    flat_queries = queries.reshape(row_total, entry_width)
    scores = (
        lax.dot_general(
            flat_queries, keys, (((1,), (1,)), ((), ())), preferred_element_type=jnp.float32
        )
        * score_scale
    )
    visible = key_positions[None, :] <= query_positions[:, None]
    masked = jnp.where(visible, scores, neg_fill)
    top_score = jnp.max(masked, axis=1)
    weights = jnp.where(visible, jnp.exp(masked - top_score[:, None]), 0.0)
    totals = jnp.sum(weights, axis=1)
    blended = jnp.dot(
        weights.astype(jnp.bfloat16), keys[:, :lat_width], preferred_element_type=jnp.float32
    )
    latent_out = (
        (blended / totals[:, None])
        .astype(jnp.bfloat16)
        .reshape(query_tokens, head_count, lat_width)
    )
    return jnp.einsum(
        "shl,hlv->shv", latent_out, w_uv, preferred_element_type=jnp.float32
    ).astype(jnp.bfloat16)


def shards(
    queries, latents, block_starts, w_uv, moe_tokens, expert_ids, gate_weights, w_gate, w_up, w_down
):
    token_count, picks = expert_ids.shape
    model_width = moe_tokens.shape[1]
    expert_count = lax.axis_size("exp")
    ctx_size = lax.axis_size("ctx")
    width = model_width // ctx_size
    capacity = 3 * token_count * picks // (2 * expert_count)
    mine = lax.axis_index("ctx").astype(jnp.int32)
    ids = expert_ids.T

    down_columns = w_down[0].reshape(w_down.shape[1], ctx_size, width)
    down_parts = []
    for offset in range(ctx_size):
        part = lax.dynamic_index_in_dim(down_columns, mine ^ offset, axis=1, keepdims=False)
        down_parts.append(part if offset == 0 else swap(part, "ctx", offset))

    outgoing = dispatch(moe_tokens, ids, capacity, expert_count)
    arrived = [outgoing[0]] + [None] * (expert_count - 1)
    for offset in range(1, expert_count):
        arrived[offset] = swap(outgoing[offset], "exp", offset)

    attended = attention(queries, latents, block_starts, w_uv)

    both_up = jnp.concatenate([w_gate[0], w_up[0]], axis=1).reshape(ctx_size, width, -1)
    up_parts = [
        lax.dynamic_index_in_dim(both_up, mine ^ offset, axis=0, keepdims=False)
        for offset in range(ctx_size)
    ]
    half = expert_count // 2
    hidden_chunks = []
    for chunk in (arrived[:half], arrived[half:]):
        pieces = gather_xor(jnp.concatenate(chunk, axis=0))
        acc = None
        for piece, part in zip(pieces, up_parts):
            term = jnp.dot(piece, part, preferred_element_type=jnp.float32)
            acc = term if acc is None else acc + term
        gate_h, up_h = jnp.split(acc, 2, axis=1)
        hidden_chunks.append((jax.nn.silu(gate_h) * up_h).astype(jnp.bfloat16))
    hidden = jnp.concatenate(hidden_chunks, axis=0)
    all_hidden = jnp.concatenate(gather_xor(hidden), axis=1)
    down_matrix = jnp.concatenate(down_parts, axis=0)
    summed = jnp.dot(all_hidden, down_matrix, preferred_element_type=jnp.float32).astype(jnp.bfloat16)
    summed = summed.reshape(expert_count, capacity, width)
    returned = [summed[0]]
    for offset in range(1, expert_count):
        returned.append(swap(summed[offset], "exp", offset))
    return attended, combine(returned, ids, gate_weights)


def solution(mesh):
    in_specs = (
        P("ctx", "exp", None),
        P("ctx", None),
        P(),
        P("exp", None, None),
        P("exp", None),
        P("exp", None),
        P("exp", None),
        P("exp", None, "ctx"),
        P("exp", None, "ctx"),
        P("exp", "ctx", None),
    )
    out_specs = (P("ctx", "exp", None), P("exp", "ctx"))
    return jax.shard_map(shards, mesh=mesh, in_specs=in_specs, out_specs=out_specs, check_vma=False)
```

```python
import functools
import math

import jax
import jax.numpy as jnp
from jax import lax
from jax.experimental import pallas as pl
from jax.experimental.pallas import tpu as pltpu
from jax.sharding import PartitionSpec as P

score_scale = (0.1 * math.log(40.0) + 1.0) ** 2 / math.sqrt(192.0)
neg_fill = -1e30
SETS = 2


def swap(x, axis, offset):
    size = lax.axis_size(axis)
    return lax.ppermute(x, axis, [(i, i ^ offset) for i in range(size)])


def after(x, *others):
    return lax.optimization_barrier((x, *others))[0]


def where_am_i():
    return jnp.stack([lax.axis_index("exp"), lax.axis_index("ctx")]).astype(jnp.int32)


def token_positions(block_starts, token_index, half_block):
    block_index = token_index // half_block
    matches = block_index[:, None] == jnp.arange(block_starts.shape[0], dtype=jnp.int32)[None, :]
    first_pos = jnp.sum(jnp.where(matches, block_starts[None, :], 0), axis=1)
    return first_pos + token_index % half_block


def whole_spec(shape):
    return pl.BlockSpec(shape, lambda i, w: (0,) * len(shape))


def call(kernel, name, grid, operands, in_specs, out_shape, out_specs, flops, where):
    shapes = jax.tree.leaves(out_shape)
    moved = sum(math.prod(x.shape) * x.dtype.itemsize for x in list(operands) + shapes)
    return pl.pallas_call(
        kernel,
        out_shape=out_shape,
        grid_spec=pltpu.PrefetchScalarGridSpec(
            num_scalar_prefetch=1, grid=grid, in_specs=in_specs, out_specs=out_specs
        ),
        cost_estimate=pl.CostEstimate(flops=flops, bytes_accessed=moved, transcendentals=0),
        name=name,
    )(where, *operands)


def split_kernel(where_ref, *refs):
    half = len(refs) // 2
    for source, target in zip(refs[:half], refs[half:]):
        target[...] = source[...]


def split_columns(matrix, width, where):
    rows, ctx_size = matrix.shape[0], matrix.shape[1] // width
    if width % 128:
        return [
            lax.dynamic_slice_in_dim(matrix, (where[1] ^ k) * width, width, axis=1)
            for k in range(1, ctx_size)
        ]
    specs = [
        pl.BlockSpec((rows, width), lambda i, w, k=k: (0, w[1] ^ k)) for k in range(1, ctx_size)
    ]
    out = jax.ShapeDtypeStruct((rows, width), matrix.dtype)
    count = ctx_size - 1
    return call(
        split_kernel, "split", (1,), [matrix] * count, specs,
        [out] * count, [whole_spec((rows, width))] * count, rows * width, where,
    )


def own_columns(matrix, width, where):
    rows = matrix.shape[0]
    if width % 128:
        return lax.dynamic_slice_in_dim(matrix, where[1] * width, width, axis=1), whole_spec((rows, width))
    return matrix, pl.BlockSpec((rows, width), lambda i, w: (0, w[1]))


def dispatch_kernel(capacity, where_ref, ids_ref, tokens_ref, *out_refs):
    expert_count = len(out_refs)
    ids = ids_ref[...]
    picks, token_count = ids.shape
    experts = lax.broadcasted_iota(jnp.int32, (expert_count, token_count), 0)
    named = jnp.zeros((expert_count, token_count), jnp.float32)
    for k in range(picks):
        named = named + jnp.where(ids[k : k + 1, :] == experts, 1.0, 0.0)
    rows = lax.broadcasted_iota(jnp.int32, (token_count, token_count), 0)
    cols = lax.broadcasted_iota(jnp.int32, (token_count, token_count), 1)
    before = jnp.where(rows < cols, 1.0, 0.0).astype(jnp.bfloat16)
    rank = jnp.dot(named.astype(jnp.bfloat16), before, preferred_element_type=jnp.float32)
    slots = lax.broadcasted_iota(jnp.int32, (expert_count * capacity, token_count), 0)
    chosen = None
    for k in range(picks):
        own = jnp.where(ids[k : k + 1, :] == experts, rank, 0.0)
        place = jnp.sum(own, axis=0, keepdims=True).astype(jnp.int32)
        place = place + (ids[k : k + 1, :] ^ where_ref[0]) * capacity
        hit = jnp.where(place == slots, 1.0, 0.0)
        chosen = hit if chosen is None else chosen + hit
    rows = jnp.dot(
        chosen.astype(jnp.bfloat16), tokens_ref[...], preferred_element_type=jnp.float32
    ).astype(tokens_ref.dtype)
    for k in range(expert_count):
        out_refs[k][...] = rows[k * capacity : (k + 1) * capacity, :]


def dispatch(tokens, ids, capacity, expert_count, width, where):
    operand, spec = own_columns(tokens, width, where)
    block = (capacity, width)
    return call(
        functools.partial(dispatch_kernel, capacity), "dispatch", (1,),
        [ids, operand], [whole_spec(ids.shape), spec],
        [jax.ShapeDtypeStruct(block, tokens.dtype)] * expert_count,
        [whole_spec(block)] * expert_count,
        2 * expert_count * capacity * tokens.shape[0] * width, where,
    )


def pack_kernel(where_ref, *refs):
    rows = refs[0].shape[0]
    for i, source in enumerate(refs[:-1]):
        refs[-1][i * rows : (i + 1) * rows, :] = source[...]


def pack(blocks, where):
    rows, width = blocks[0].shape
    shape = (len(blocks) * rows, width)
    return call(
        pack_kernel, "pack", (1,), blocks, [whole_spec((rows, width))] * len(blocks),
        jax.ShapeDtypeStruct(shape, blocks[0].dtype), whole_spec(shape), shape[0] * width, where,
    )


def mlp_kernel(where_ref, gate_ref, up_ref, *refs):
    pieces, out_ref = refs[:-1], refs[-1]
    width = pieces[0].shape[1]
    acc = None
    for j, piece in enumerate(pieces):
        at = pl.ds(pl.multiple_of((where_ref[1] ^ j) * width, 16), width)
        weights = jnp.concatenate([gate_ref[at, :], up_ref[at, :]], axis=1)
        term = jnp.dot(piece[...], weights, preferred_element_type=jnp.float32)
        acc = term if acc is None else acc + term
    hidden_width = gate_ref.shape[1]
    gate_h, up_h = acc[:, :hidden_width], acc[:, hidden_width:]
    out_ref[...] = (gate_h / (1.0 + jnp.exp(-gate_h)) * up_h).astype(out_ref.dtype)


def mlp(pieces, gate_matrix, up_matrix, where):
    rows, width = pieces[0].shape
    shape = (rows, gate_matrix.shape[1])
    return call(
        mlp_kernel, "mlp", (1,), [gate_matrix, up_matrix, *pieces],
        [whole_spec(gate_matrix.shape)] * 2 + [whole_spec((rows, width))] * len(pieces),
        jax.ShapeDtypeStruct(shape, pieces[0].dtype), whole_spec(shape),
        4 * rows * math.prod(gate_matrix.shape), where,
    )


def down_kernel(where_ref, hidden_ref, *refs):
    ctx_size = hidden_ref.shape[0]
    parts, out_refs = refs[:ctx_size], refs[ctx_size:]
    rows = out_refs[0].shape[0]
    hidden = jnp.concatenate([hidden_ref[where_ref[1] ^ j] for j in range(ctx_size)], axis=1)
    matrix = jnp.concatenate([part[...] for part in parts], axis=0)
    out = jnp.dot(hidden, matrix, preferred_element_type=jnp.float32).astype(out_refs[0].dtype)
    for i, target in enumerate(out_refs):
        target[...] = out[i * rows : (i + 1) * rows, :]


def down(hidden, own, others, block_count, where):
    width = others[0].shape[1]
    operand, spec = own_columns(own, width, where)
    block = (hidden.shape[1] // block_count, width)
    return call(
        down_kernel, "down", (1,), [hidden, operand, *others],
        [whole_spec(hidden.shape), spec] + [whole_spec(others[0].shape)] * len(others),
        [jax.ShapeDtypeStruct(block, hidden.dtype)] * block_count,
        [whole_spec(block)] * block_count,
        2 * math.prod(hidden.shape) * width, where,
    )


def combine_kernel(where_ref, ids_ref, gates_ref, *refs):
    row_refs, out_ref = refs[:-1], refs[-1]
    expert_count, capacity = len(row_refs), row_refs[0].shape[0]
    ids, gates = ids_ref[...], gates_ref[...]
    token_count, picks = ids.shape
    experts = lax.broadcasted_iota(jnp.int32, (token_count, expert_count), 1)
    named = jnp.zeros((token_count, expert_count), jnp.float32)
    for k in range(picks):
        named = named + jnp.where(ids[:, k : k + 1] == experts, 1.0, 0.0)
    rows = lax.broadcasted_iota(jnp.int32, (token_count, token_count), 0)
    cols = lax.broadcasted_iota(jnp.int32, (token_count, token_count), 1)
    before = jnp.where(cols < rows, 1.0, 0.0).astype(jnp.bfloat16)
    rank = jnp.dot(before, named.astype(jnp.bfloat16), preferred_element_type=jnp.float32)
    slots = lax.broadcasted_iota(jnp.int32, (token_count, expert_count * capacity), 1)
    hits = []
    for k in range(picks):
        own = jnp.where(ids[:, k : k + 1] == experts, rank, 0.0)
        place = jnp.sum(own, axis=1, keepdims=True).astype(jnp.int32)
        place = place + (ids[:, k : k + 1] ^ where_ref[0]) * capacity
        hits.append(jnp.where(place == slots, 1.0, 0.0).astype(jnp.bfloat16))
    arrived = jnp.concatenate([ref[...] for ref in row_refs], axis=0)
    chosen = jnp.dot(
        jnp.concatenate(hits, axis=0), arrived, preferred_element_type=jnp.float32
    )
    total = None
    for k in range(picks):
        term = chosen[k * token_count : (k + 1) * token_count, :] * gates[:, k : k + 1]
        total = term if total is None else total + term
    out_ref[...] = total.astype(out_ref.dtype)


def combine(row_blocks, ids, gates, where):
    capacity, width = row_blocks[0].shape
    token_count, picks = ids.shape
    expert_count = len(row_blocks)
    steps = 1 if width % 256 else 2
    part = width // steps
    row_spec = pl.BlockSpec((capacity, part), lambda i, w: (0, i))
    return call(
        combine_kernel, "combine", (steps,), [ids, gates, *row_blocks],
        [whole_spec(ids.shape), whole_spec(gates.shape)] + [row_spec] * expert_count,
        jax.ShapeDtypeStruct((token_count, width), row_blocks[0].dtype),
        pl.BlockSpec((token_count, part), lambda i, w: (0, i)),
        2 * picks * expert_count * capacity * token_count * width, where,
    )


def attention(queries, keys, block_starts, w_uv):
    query_tokens, head_count, entry_width = queries.shape
    lat_width = w_uv.shape[1]
    half_block = query_tokens // 2
    row_total = query_tokens * head_count
    mine = lax.axis_index("ctx").astype(jnp.int32)
    ctx_size = lax.axis_size("ctx")
    offsets = jnp.arange(query_tokens, dtype=jnp.int32)
    own_positions = token_positions(block_starts, mine * query_tokens + offsets, half_block)
    query_positions = jnp.repeat(own_positions, head_count)
    owners = jnp.bitwise_xor(mine, jnp.arange(ctx_size, dtype=jnp.int32))
    key_index = (owners[:, None] * query_tokens + offsets[None, :]).reshape(-1)
    key_positions = token_positions(block_starts, key_index, half_block)
    flat_queries = queries.reshape(row_total, entry_width)
    scores = (
        lax.dot_general(
            flat_queries, keys, (((1,), (1,)), ((), ())), preferred_element_type=jnp.float32
        )
        * score_scale
    )
    visible = key_positions[None, :] <= query_positions[:, None]
    masked = jnp.where(visible, scores, neg_fill)
    top_score = jnp.max(masked, axis=1)
    weights = jnp.where(visible, jnp.exp(masked - top_score[:, None]), 0.0)
    totals = jnp.sum(weights, axis=1)
    blended = jnp.dot(
        weights.astype(jnp.bfloat16), keys[:, :lat_width], preferred_element_type=jnp.float32
    )
    latent_out = (
        (blended / totals[:, None])
        .astype(jnp.bfloat16)
        .reshape(query_tokens, head_count, lat_width)
    )
    return jnp.einsum(
        "shl,hlv->shv", latent_out, w_uv, preferred_element_type=jnp.float32
    ).astype(jnp.bfloat16)


def shards(
    queries, latents, block_starts, w_uv, moe_tokens, expert_ids, gate_weights, w_gate, w_up, w_down
):
    token_count, picks = expert_ids.shape
    expert_count = lax.axis_size("exp")
    ctx_size = lax.axis_size("ctx")
    width = moe_tokens.shape[1] // ctx_size
    capacity = 3 * token_count * picks // (2 * expert_count)
    where = where_am_i()
    evens = range(2, ctx_size, 2)

    slices = split_columns(w_down[0], width, where)
    order = list(evens) + [k for k in range(1, ctx_size, 2)]
    down_parts = [None] * ctx_size
    for offset in sorted(range(1, ctx_size), reverse=True):
        down_parts[offset] = swap(slices[offset - 1], "ctx", offset)

    outgoing = dispatch(moe_tokens, expert_ids.T, capacity, expert_count, width, where)
    half = expert_count // 2
    sets = [
        [k for k in range(expert_count) if (k % half) * SETS // half == s] for s in range(SETS)
    ]
    arrived = [None] * expert_count
    for members in sets:
        for k in sorted(members, reverse=True):
            arrived[k] = swap(outgoing[k], "exp", k) if k else outgoing[0]

    returned = [None] * expert_count
    packed = [pack([arrived[k] for k in members], where) for members in sets]
    for members, rows in zip(sets, packed):
        pieces = [rows] + [None] * (ctx_size - 1)
        for offset in evens:
            pieces[offset] = swap(rows, "ctx", offset)
        for offset in range(0, ctx_size, 2):
            pieces[offset + 1] = swap(pieces[offset], "ctx", 1)
        hidden = mlp(pieces, w_gate[0], w_up[0], where)
        hidden = lax.all_gather(hidden, "ctx", axis=0)
        blocks = down(hidden, w_down[0], down_parts[1:], len(members), where)
        for k, block in sorted(zip(members, blocks), key=lambda pair: -pair[0]):
            returned[k] = swap(block, "exp", k) if k else block

    near = after(latents, packed[-1])
    keys = [near] + [None] * (ctx_size - 1)
    for offset in evens:
        keys[offset] = swap(near, "ctx", offset)
    for offset in range(0, ctx_size, 2):
        keys[offset + 1] = swap(keys[offset], "ctx", 1)
    attended = attention(queries, jnp.concatenate(keys, axis=0), block_starts, w_uv)
    return attended, combine(returned, expert_ids, gate_weights, where)


def solution(mesh):
    in_specs = (
        P("ctx", "exp", None),
        P("ctx", None),
        P(),
        P("exp", None, None),
        P("exp", None),
        P("exp", None),
        P("exp", None),
        P("exp", None, "ctx"),
        P("exp", None, "ctx"),
        P("exp", "ctx", None),
    )
    out_specs = (P("ctx", "exp", None), P("exp", "ctx"))
    return jax.shard_map(shards, mesh=mesh, in_specs=in_specs, out_specs=out_specs, check_vma=False)
```

```python
import functools
import math

import jax
import jax.numpy as jnp
from jax import lax
from jax.experimental import pallas as pl
from jax.experimental.pallas import tpu as pltpu
from jax.sharding import PartitionSpec as P


score_scale = (0.1 * math.log(40.0) + 1.0) ** 2 / math.sqrt(192.0)
neg_fill = -1e30
SETS = 2


def swap(x, axis, offset):
    size = lax.axis_size(axis)
    return lax.ppermute(x, axis, [(i, i ^ offset) for i in range(size)])


def set_members(expert_count):
    half = expert_count // 2
    return [
        [k for k in range(expert_count) if (k % half) * SETS // half == s] for s in range(SETS)
    ]


def where_am_i():
    return jnp.stack([lax.axis_index("exp"), lax.axis_index("ctx")]).astype(jnp.int32)


def whole_spec(shape):
    return pl.BlockSpec(shape, lambda i, *_: (0,) * len(shape))


def call(kernel, grid, operands, in_specs, out_shape, out_specs, flops, scalars, vmem=16 << 20, scratch=()):
    scalars = scalars if isinstance(scalars, tuple) else (scalars,)
    shapes = jax.tree.leaves(out_shape)
    moved = sum(math.prod(x.shape) * x.dtype.itemsize for x in list(operands) + shapes)
    return pl.pallas_call(
        kernel,
        out_shape=out_shape,
        grid_spec=pltpu.PrefetchScalarGridSpec(
            num_scalar_prefetch=len(scalars), grid=grid, in_specs=in_specs, out_specs=out_specs,
            scratch_shapes=scratch,
        ),
        cost_estimate=pl.CostEstimate(flops=flops, bytes_accessed=moved, transcendentals=0),
        compiler_params=pltpu.CompilerParams(vmem_limit_bytes=vmem),
    )(*scalars, *operands)


def split_kernel(where_ref, *refs):
    half = len(refs) // 2
    for source, target in zip(refs[:half], refs[half:]):
        target[...] = source[...]


def split_columns(matrix, width, where):
    rows, ctx_size = matrix.shape[0], matrix.shape[1] // width
    count = ctx_size - 1
    operands = [matrix] * count
    specs = [
        pl.BlockSpec((rows, width), lambda i, w, k=k: (0, w[1] ^ k)) for k in range(1, ctx_size)
    ]
    if width % 128:
        specs = [whole_spec((rows, width))] * count
        operands = [
            lax.dynamic_slice_in_dim(matrix, (where[1] ^ k) * width, width, axis=1)
            for k in range(1, ctx_size)
        ]
    out = jax.ShapeDtypeStruct((rows, width), matrix.dtype)
    return call(
        split_kernel, (1,), operands, specs,
        [out] * count, [whole_spec((rows, width))] * count, rows * width, where,
    )


def own_columns(matrix, width, where):
    rows = matrix.shape[0]
    if width % 128:
        return lax.dynamic_slice_in_dim(matrix, where[1] * width, width, axis=1), whole_spec((rows, width))
    return matrix, pl.BlockSpec((rows, width), lambda i, w: (0, w[1]))


def dispatch_kernel(capacity, where_ref, ids_ref, tokens_ref, *out_refs):
    expert_count = len(out_refs)
    ids = ids_ref[...]
    picks, token_count = ids.shape
    experts = lax.broadcasted_iota(jnp.int32, (expert_count, token_count), 0)
    named = jnp.zeros((expert_count, token_count), jnp.float32)
    for k in range(picks):
        named = named + jnp.where(ids[k : k + 1, :] == experts, 1.0, 0.0)
    rows = lax.broadcasted_iota(jnp.int32, (token_count, token_count), 0)
    cols = lax.broadcasted_iota(jnp.int32, (token_count, token_count), 1)
    before = jnp.where(rows < cols, 1.0, 0.0).astype(jnp.bfloat16)
    rank = jnp.dot(named.astype(jnp.bfloat16), before, preferred_element_type=jnp.float32)
    slots = lax.broadcasted_iota(jnp.int32, (expert_count * capacity, token_count), 0)
    chosen = None
    for k in range(picks):
        own = jnp.where(ids[k : k + 1, :] == experts, rank, 0.0)
        place = jnp.sum(own, axis=0, keepdims=True).astype(jnp.int32)
        place = place + (ids[k : k + 1, :] ^ where_ref[0]) * capacity
        hit = jnp.where(place == slots, 1.0, 0.0)
        chosen = hit if chosen is None else chosen + hit
    rows = jnp.dot(
        chosen.astype(jnp.bfloat16), tokens_ref[...], preferred_element_type=jnp.float32
    ).astype(tokens_ref.dtype)
    for k in range(expert_count):
        out_refs[k][...] = rows[k * capacity : (k + 1) * capacity, :]


def dispatch(tokens, ids, capacity, expert_count, width, where):
    operand, spec = own_columns(tokens, width, where)
    block = (capacity, width)
    return call(
        functools.partial(dispatch_kernel, capacity), (1,),
        [ids, operand], [whole_spec(ids.shape), spec],
        [jax.ShapeDtypeStruct(block, tokens.dtype)] * expert_count,
        [whole_spec(block)] * expert_count,
        2 * expert_count * capacity * tokens.shape[0] * width, where,
    )


def pack_kernel(where_ref, *refs):
    rows = refs[0].shape[0]
    for i, source in enumerate(refs[:-1]):
        refs[-1][i * rows : (i + 1) * rows, :] = source[...]


def pack(blocks, where):
    rows, width = blocks[0].shape
    shape = (len(blocks) * rows, width)
    return call(
        pack_kernel, (1,), blocks, [whole_spec((rows, width))] * len(blocks),
        jax.ShapeDtypeStruct(shape, blocks[0].dtype), whole_spec(shape), shape[0] * width, where,
    )


def up_sum(gate_refs, up_refs, pieces):
    acc = None
    for gate_ref, up_ref, piece in zip(gate_refs, up_refs, pieces):
        weights = jnp.concatenate([gate_ref[...], up_ref[...]], axis=1)
        term = jnp.dot(piece[...], weights, preferred_element_type=jnp.float32)
        acc = term if acc is None else acc + term
    return acc


def part_kernel(where_ref, *refs):
    count = len(refs) // 3
    refs[-1][...] = up_sum(refs[:count], refs[count : 2 * count], refs[2 * count : -1])


def mlp_kernel(where_ref, *refs):
    count = len(refs) // 3
    acc = refs[-2][...] + up_sum(refs[:count], refs[count : 2 * count], refs[2 * count : -2])
    hidden_width = acc.shape[1] // 2
    gate_h, up_h = acc[:, :hidden_width], acc[:, hidden_width:]
    refs[-1][...] = (gate_h / (1.0 + jnp.exp(-gate_h)) * up_h).astype(refs[-1].dtype)


def mlp(pieces, offsets, gate_matrix, up_matrix, partial, where):
    rows, width = pieces[0].shape
    count, hidden_width = len(pieces), gate_matrix.shape[1]
    specs = [
        pl.BlockSpec((width, hidden_width), lambda i, w, k=k: (w[1] ^ k, 0)) for k in offsets
    ]
    operands = [gate_matrix] * count + [up_matrix] * count + list(pieces)
    specs = specs + specs + [whole_spec((rows, width))] * count
    if partial is None:
        kernel, out = part_kernel, jax.ShapeDtypeStruct((rows, 2 * hidden_width), jnp.float32)
    else:
        kernel, out = mlp_kernel, jax.ShapeDtypeStruct((rows, hidden_width), pieces[0].dtype)
        operands.append(partial)
        specs.append(whole_spec(partial.shape))
    return call(
        kernel, (1,), operands, specs, out, whole_spec(out.shape),
        4 * count * rows * width * hidden_width, where, vmem=24 << 20,
    )


def tiles(width):
    step = 256 if width % 256 == 0 else width
    return [slice(at, at + step) for at in range(0, width, step)]


def down_kernel(where_ref, hidden_ref, *refs):
    ctx_size = hidden_ref.shape[0]
    parts, out_refs = refs[:ctx_size], refs[ctx_size:]
    rows, width = out_refs[0].shape
    hidden = jnp.concatenate([hidden_ref[where_ref[1] ^ j] for j in range(ctx_size)], axis=1)
    for tile in tiles(width):
        matrix = jnp.concatenate([part[:, tile] for part in parts], axis=0)
        out = jnp.dot(hidden, matrix, preferred_element_type=jnp.float32)
        out = out.astype(out_refs[0].dtype)
        for i, target in enumerate(out_refs):
            target[:, tile] = out[i * rows : (i + 1) * rows, :]


def down(hidden, own, others, block_count, where):
    width = others[0].shape[1]
    operand, spec = own_columns(own, width, where)
    block = (hidden.shape[1] // block_count, width)
    return call(
        down_kernel, (1,), [hidden, operand, *others],
        [whole_spec(hidden.shape), spec] + [whole_spec(others[0].shape)] * len(others),
        [jax.ShapeDtypeStruct(block, hidden.dtype)] * block_count,
        [whole_spec(block)] * block_count,
        2 * math.prod(hidden.shape) * width, where,
    )


def combine_kernel(where_ref, ids_ref, gates_ref, *refs):
    row_refs, out_ref = refs[:-1], refs[-1]
    expert_count, capacity = len(row_refs), row_refs[0].shape[0]
    picks, token_count = ids_ref.shape
    columns = jnp.concatenate(
        [ids_ref[...].astype(jnp.float32), gates_ref[...]]
        + [jnp.zeros((-2 * picks % 8, token_count), jnp.float32)],
        axis=0,
    ).T
    ids, gates = columns[:, :picks].astype(jnp.int32), columns[:, picks : 2 * picks]
    experts = lax.broadcasted_iota(jnp.int32, (token_count, expert_count), 1)
    named = jnp.zeros((token_count, expert_count), jnp.float32)
    for k in range(picks):
        named = named + jnp.where(ids[:, k : k + 1] == experts, 1.0, 0.0)
    rows = lax.broadcasted_iota(jnp.int32, (token_count, token_count), 0)
    cols = lax.broadcasted_iota(jnp.int32, (token_count, token_count), 1)
    before = jnp.where(cols < rows, 1.0, 0.0).astype(jnp.bfloat16)
    rank = jnp.dot(before, named.astype(jnp.bfloat16), preferred_element_type=jnp.float32)
    slots = lax.broadcasted_iota(jnp.int32, (token_count, expert_count * capacity), 1)
    hits = []
    for k in range(picks):
        own = jnp.where(ids[:, k : k + 1] == experts, rank, 0.0)
        place = jnp.sum(own, axis=1, keepdims=True).astype(jnp.int32)
        place = place + (ids[:, k : k + 1] ^ where_ref[0]) * capacity
        hits.append(jnp.where(place == slots, 1.0, 0.0).astype(jnp.bfloat16))
    hits = jnp.concatenate(hits, axis=0)
    for tile in tiles(out_ref.shape[1]):
        arrived = jnp.concatenate([ref[:, tile] for ref in row_refs], axis=0)
        chosen = jnp.dot(hits, arrived, preferred_element_type=jnp.float32)
        total = None
        for k in range(picks):
            term = chosen[k * token_count : (k + 1) * token_count, :] * gates[:, k : k + 1]
            total = term if total is None else total + term
        out_ref[:, tile] = total.astype(out_ref.dtype)


def combine(row_blocks, ids, gates, where):
    capacity, width = row_blocks[0].shape
    picks, token_count = ids.shape
    expert_count = len(row_blocks)
    out = jax.ShapeDtypeStruct((token_count, width), row_blocks[0].dtype)
    return call(
        combine_kernel, (1,), [ids, gates, *row_blocks],
        [whole_spec(ids.shape), whole_spec(gates.shape)]
        + [whole_spec((capacity, width))] * expert_count,
        out, whole_spec(out.shape),
        2 * picks * expert_count * capacity * token_count * width, where,
    )


def block_positions(starts_ref, owner, count, axis):
    shape = (count, 1) if axis == 0 else (1, count)
    index = lax.broadcasted_iota(jnp.int32, shape, axis)
    half = count // 2
    first, second = starts_ref[2 * owner], starts_ref[2 * owner + 1]
    return jnp.where(index < half, first + index, second + index - half)


def attention_kernel(where_ref, starts_ref, queries_ref, uv_ref, *refs):
    keys, out_ref, flipped, joined, late = refs[:-4], refs[-4], refs[-3], refs[-2], refs[-1]
    token_count = queries_ref.shape[2]
    lat_width = uv_ref.shape[1]
    query_positions = block_positions(starts_ref, where_ref[1], token_count, 1)
    for j, block in enumerate(keys):
        at = slice(j * token_count, (j + 1) * token_count)
        flipped[:, at] = block[...]
        joined[at, :] = block[...].T
        key_positions = block_positions(starts_ref, where_ref[1] ^ j, token_count, 0)
        late[at, :] = jnp.where(key_positions <= query_positions, 0.0, neg_fill)

    @pl.loop(0, queries_ref.shape[0])
    def _(head):
        scores = jnp.dot(joined[...], queries_ref[head], preferred_element_type=jnp.float32)
        hidden = late[...] < 0.0
        masked = jnp.where(hidden, neg_fill, scores * score_scale)
        top_score = jnp.max(masked, axis=0, keepdims=True)
        weights = jnp.where(hidden, 0.0, jnp.exp(masked - top_score))
        totals = jnp.sum(weights, axis=0, keepdims=True)
        blended = jnp.dot(
            flipped[:lat_width, :], weights.astype(jnp.bfloat16), preferred_element_type=jnp.float32
        )
        latent_out = (blended / totals).astype(jnp.bfloat16)
        out_ref[head] = lax.dot_general(
            latent_out, uv_ref[head], (((0,), (0,)), ((), ())), preferred_element_type=jnp.float32
        ).astype(out_ref.dtype)


def attention(queries, keys, block_starts, w_uv, where):
    head_count, entry_width, token_count = queries.shape
    key_count = len(keys) * token_count
    shape = (head_count, token_count, w_uv.shape[2])
    return call(
        attention_kernel, (1,), [queries, w_uv, *keys],
        [whole_spec(queries.shape), whole_spec(w_uv.shape)]
        + [whole_spec((entry_width, token_count))] * len(keys),
        jax.ShapeDtypeStruct(shape, queries.dtype), whole_spec(shape),
        4 * head_count * key_count * token_count * entry_width, (where, block_starts),
        vmem=24 << 20,
        scratch=[
            pltpu.VMEM((entry_width, key_count), queries.dtype),
            pltpu.VMEM((key_count, entry_width), queries.dtype),
            pltpu.VMEM((key_count, token_count), jnp.float32),
        ],
    )


def layer(
    queries, latents, block_starts, w_uv, moe_tokens, expert_ids, gate_weights, w_gate, w_up, w_down
):
    token_count, picks = expert_ids.shape
    expert_count = lax.axis_size("exp")
    ctx_size = lax.axis_size("ctx")
    width = moe_tokens.shape[1] // ctx_size
    capacity = 3 * token_count * picks // (2 * expert_count)
    where = where_am_i()
    evens = range(2, ctx_size, 2)

    slices = split_columns(w_down[0], width, where)
    down_parts = [swap(slices[offset - 1], "ctx", offset) for offset in range(1, ctx_size)]

    outgoing = dispatch(moe_tokens, expert_ids.T, capacity, expert_count, width, where)
    sets = set_members(expert_count)
    arrived = [swap(outgoing[k], "exp", k) if k else outgoing[0] for k in range(expert_count)]

    returned = [None] * expert_count
    for members in sets:
        pieces = [None] * ctx_size
        pieces[0] = pack([arrived[k] for k in members], where)
        for offset in evens:
            pieces[offset] = swap(pieces[0], "ctx", offset)
        for offset in range(0, ctx_size, 2):
            pieces[offset + 1] = swap(pieces[offset], "ctx", 1)
        partial = mlp(pieces[:2], [0, 1], w_gate[0], w_up[0], None, where)
        hidden = mlp(pieces[2:], range(2, ctx_size), w_gate[0], w_up[0], partial, where)
        hidden = lax.all_gather(hidden, "ctx", axis=0)
        blocks = down(hidden, w_down[0], down_parts, len(members), where)
        for k, block in zip(members, blocks):
            returned[k] = swap(block, "exp", k) if k else block

    keys = [latents.T] + [None] * (ctx_size - 1)
    for offset in evens:
        keys[offset] = swap(keys[0], "ctx", offset)
    for offset in range(0, ctx_size, 2):
        keys[offset + 1] = swap(keys[offset], "ctx", 1)
    attended = attention(jnp.transpose(queries, (1, 2, 0)), keys, block_starts, w_uv, where)
    attended = jnp.transpose(attended, (1, 0, 2))
    return attended, combine(returned, expert_ids.T, gate_weights.T, where)


def solution(mesh):
    in_specs = (
        P("ctx", "exp", None),
        P("ctx", None),
        P(),
        P("exp", None, None),
        P("exp", None),
        P("exp", None),
        P("exp", None),
        P("exp", None, "ctx"),
        P("exp", None, "ctx"),
        P("exp", "ctx", None),
    )
    out_specs = (P("ctx", "exp", None), P("exp", "ctx"))
    return jax.shard_map(layer, mesh=mesh, in_specs=in_specs, out_specs=out_specs, check_vma=False)
```

```python
import functools
import math

import jax
import jax.numpy as jnp
from jax import lax
from jax.experimental import pallas as pl
from jax.experimental.pallas import tpu as pltpu
from jax.sharding import PartitionSpec as P


score_scale = (0.1 * math.log(40.0) + 1.0) ** 2 / math.sqrt(192.0)
neg_fill = -1e30
SETS = 2
CHUNKS = (1, 2)


def swap(x, axis, offset):
    size = lax.axis_size(axis)
    return lax.ppermute(x, axis, [(i, i ^ offset) for i in range(size)])


def set_members(expert_count):
    half = expert_count // 2
    return [
        [k for k in range(expert_count) if (k % half) * SETS // half == s]
        for s in reversed(range(SETS))
    ]


def where_am_i():
    return jnp.stack([lax.axis_index("exp"), lax.axis_index("ctx")]).astype(jnp.int32)


def whole_spec(shape):
    return pl.BlockSpec(shape, lambda i, *_: (0,) * len(shape))


def call(kernel, grid, operands, in_specs, out_shape, out_specs, flops, scalars, vmem=16 << 20, scratch=()):
    scalars = scalars if isinstance(scalars, tuple) else (scalars,)
    shapes = jax.tree.leaves(out_shape)
    moved = sum(math.prod(x.shape) * x.dtype.itemsize for x in list(operands) + shapes)
    return pl.pallas_call(
        kernel,
        out_shape=out_shape,
        grid_spec=pltpu.PrefetchScalarGridSpec(
            num_scalar_prefetch=len(scalars), grid=grid, in_specs=in_specs, out_specs=out_specs,
            scratch_shapes=scratch,
        ),
        cost_estimate=pl.CostEstimate(flops=flops, bytes_accessed=moved, transcendentals=0),
        compiler_params=pltpu.CompilerParams(vmem_limit_bytes=vmem),
    )(*scalars, *operands)


def split_kernel(where_ref, *refs):
    half = len(refs) // 2
    for source, target in zip(refs[:half], refs[half:]):
        target[...] = source[...]


def split_columns(matrix, width, where):
    rows, ctx_size = matrix.shape[0], matrix.shape[1] // width
    count = ctx_size - 1
    operands = [matrix] * count
    specs = [
        pl.BlockSpec((rows, width), lambda i, w, k=k: (0, w[1] ^ k)) for k in range(1, ctx_size)
    ]
    if width % 128:
        specs = [whole_spec((rows, width))] * count
        operands = [
            lax.dynamic_slice_in_dim(matrix, (where[1] ^ k) * width, width, axis=1)
            for k in range(1, ctx_size)
        ]
    out = jax.ShapeDtypeStruct((rows, width), matrix.dtype)
    return call(
        split_kernel, (1,), operands, specs,
        [out] * count, [whole_spec((rows, width))] * count, rows * width, where,
    )


def own_columns(matrix, width, where):
    rows = matrix.shape[0]
    if width % 128:
        return lax.dynamic_slice_in_dim(matrix, where[1] * width, width, axis=1), whole_spec((rows, width))
    return matrix, pl.BlockSpec((rows, width), lambda i, w: (0, w[1]))


def dispatch_kernel(capacity, where_ref, ids_ref, tokens_ref, *out_refs):
    expert_count = len(out_refs)
    ids = ids_ref[...]
    picks, token_count = ids.shape
    experts = lax.broadcasted_iota(jnp.int32, (expert_count, token_count), 0)
    named = jnp.zeros((expert_count, token_count), jnp.float32)
    for k in range(picks):
        named = named + jnp.where(ids[k : k + 1, :] == experts, 1.0, 0.0)
    rows = lax.broadcasted_iota(jnp.int32, (token_count, token_count), 0)
    cols = lax.broadcasted_iota(jnp.int32, (token_count, token_count), 1)
    before = jnp.where(rows < cols, 1.0, 0.0).astype(jnp.bfloat16)
    rank = jnp.dot(named.astype(jnp.bfloat16), before, preferred_element_type=jnp.float32)
    slots = lax.broadcasted_iota(jnp.int32, (expert_count * capacity, token_count), 0)
    chosen = None
    for k in range(picks):
        own = jnp.where(ids[k : k + 1, :] == experts, rank, 0.0)
        place = jnp.sum(own, axis=0, keepdims=True).astype(jnp.int32)
        place = place + (ids[k : k + 1, :] ^ where_ref[0]) * capacity
        hit = jnp.where(place == slots, 1.0, 0.0)
        chosen = hit if chosen is None else chosen + hit
    rows = jnp.dot(
        chosen.astype(jnp.bfloat16), tokens_ref[...], preferred_element_type=jnp.float32
    ).astype(tokens_ref.dtype)
    for k in range(expert_count):
        out_refs[k][...] = rows[k * capacity : (k + 1) * capacity, :]


def dispatch(tokens, ids, capacity, expert_count, width, where):
    operand, spec = own_columns(tokens, width, where)
    block = (capacity, width)
    return call(
        functools.partial(dispatch_kernel, capacity), (1,),
        [ids, operand], [whole_spec(ids.shape), spec],
        [jax.ShapeDtypeStruct(block, tokens.dtype)] * expert_count,
        [whole_spec(block)] * expert_count,
        2 * expert_count * capacity * tokens.shape[0] * width, where,
    )


def pack_kernel(count, where_ref, *refs):
    rows, targets = refs[0].shape[0], refs[count:]
    share = count // len(targets)
    for i, source in enumerate(refs[:count]):
        at = i % share * rows
        targets[i // share][at : at + rows, :] = source[...]


def pack(blocks, chunks, where):
    rows, width = blocks[0].shape
    shape = (len(blocks) // chunks * rows, width)
    return call(
        functools.partial(pack_kernel, len(blocks)), (1,), blocks,
        [whole_spec((rows, width))] * len(blocks),
        [jax.ShapeDtypeStruct(shape, blocks[0].dtype)] * chunks, [whole_spec(shape)] * chunks,
        len(blocks) * rows * width, where,
    )


def up_sum(count, refs):
    gate_refs, up_refs, rows = refs[:count], refs[count : 2 * count], refs[2 * count :]
    chunks = len(rows) // count
    acc = None
    for j in range(count):
        weights = jnp.concatenate([gate_refs[j][...], up_refs[j][...]], axis=1)
        piece = [ref[...] for ref in rows[j * chunks : (j + 1) * chunks]]
        piece = piece[0] if chunks == 1 else jnp.concatenate(piece, axis=0)
        term = jnp.dot(piece, weights, preferred_element_type=jnp.float32)
        acc = term if acc is None else acc + term
    return acc


def part_kernel(count, where_ref, *refs):
    refs[-1][...] = up_sum(count, refs[:-1])


def mlp_kernel(count, where_ref, *refs):
    acc = refs[-2][...] + up_sum(count, refs[:-2])
    hidden_width = acc.shape[1] // 2
    gate_h, up_h = acc[:, :hidden_width], acc[:, hidden_width:]
    refs[-1][...] = (gate_h / (1.0 + jnp.exp(-gate_h)) * up_h).astype(refs[-1].dtype)


def mlp(pieces, offsets, gate_matrix, up_matrix, partial, where):
    chunk_rows, width = pieces[0][0].shape
    count, hidden_width = len(pieces), gate_matrix.shape[1]
    rows = chunk_rows * len(pieces[0])
    flat = [chunk for piece in pieces for chunk in piece]
    specs = [
        pl.BlockSpec((width, hidden_width), lambda i, w, k=k: (w[1] ^ k, 0)) for k in offsets
    ]
    operands = [gate_matrix] * count + [up_matrix] * count + flat
    specs = specs + specs + [whole_spec((chunk_rows, width))] * len(flat)
    if partial is None:
        kernel, out = part_kernel, jax.ShapeDtypeStruct((rows, 2 * hidden_width), jnp.float32)
    else:
        kernel, out = mlp_kernel, jax.ShapeDtypeStruct((rows, hidden_width), flat[0].dtype)
        operands.append(partial)
        specs.append(whole_spec(partial.shape))
    return call(
        functools.partial(kernel, count), (1,), operands, specs, out, whole_spec(out.shape),
        4 * count * rows * width * hidden_width, where, vmem=24 << 20,
    )


def tiles(width):
    step = 256 if width % 256 == 0 else width
    return [slice(at, at + step) for at in range(0, width, step)]


def down_kernel(count, where_ref, *refs):
    parts, out_refs = refs[count : 2 * count], refs[2 * count :]
    rows, width = out_refs[0].shape
    hidden = jnp.concatenate([ref[...] for ref in refs[:count]], axis=1)
    for tile in tiles(width):
        matrix = jnp.concatenate([part[:, tile] for part in parts], axis=0)
        out = jnp.dot(hidden, matrix, preferred_element_type=jnp.float32)
        out = out.astype(out_refs[0].dtype)
        for i, target in enumerate(out_refs):
            target[:, tile] = out[i * rows : (i + 1) * rows, :]


def down(hidden, own, others, block_count, where):
    width, count = others[0].shape[1], len(hidden)
    operand, spec = own_columns(own, width, where)
    block = (hidden[0].shape[0] // block_count, width)
    return call(
        functools.partial(down_kernel, count), (1,), [*hidden, operand, *others],
        [whole_spec(hidden[0].shape)] * count + [spec] + [whole_spec(others[0].shape)] * len(others),
        [jax.ShapeDtypeStruct(block, hidden[0].dtype)] * block_count,
        [whole_spec(block)] * block_count,
        2 * count * math.prod(hidden[0].shape) * width, where,
    )


def mix(hits, gates, row_refs, tile, picks):
    token_count = hits.shape[0] // picks
    arrived = jnp.concatenate([ref[:, tile] for ref in row_refs], axis=0)
    chosen = jnp.dot(hits, arrived, preferred_element_type=jnp.float32)
    total = None
    for k in range(picks):
        term = chosen[k * token_count : (k + 1) * token_count, :] * gates[:, k : k + 1]
        total = term if total is None else total + term
    return total


def begin_kernel(members, where_ref, ids_ref, gates_ref, *refs):
    row_refs, sum_ref, hits_ref, columns_ref = refs[:-3], refs[-3], refs[-2], refs[-1]
    expert_count, capacity = sum(len(m) for m in members), row_refs[0].shape[0]
    picks, token_count = ids_ref.shape
    columns = jnp.concatenate(
        [ids_ref[...].astype(jnp.float32), gates_ref[...]]
        + [jnp.zeros((-2 * picks % 8, token_count), jnp.float32)],
        axis=0,
    ).T
    columns_ref[...] = columns
    ids, gates = columns[:, :picks].astype(jnp.int32), columns[:, picks : 2 * picks]
    experts = lax.broadcasted_iota(jnp.int32, (token_count, expert_count), 1)
    named = jnp.zeros((token_count, expert_count), jnp.float32)
    for k in range(picks):
        named = named + jnp.where(ids[:, k : k + 1] == experts, 1.0, 0.0)
    rows = lax.broadcasted_iota(jnp.int32, (token_count, token_count), 0)
    cols = lax.broadcasted_iota(jnp.int32, (token_count, token_count), 1)
    before = jnp.where(cols < rows, 1.0, 0.0).astype(jnp.bfloat16)
    rank = jnp.dot(before, named.astype(jnp.bfloat16), preferred_element_type=jnp.float32)
    places = []
    for k in range(picks):
        own = jnp.where(ids[:, k : k + 1] == experts, rank, 0.0)
        rank_k = jnp.sum(own, axis=1, keepdims=True).astype(jnp.int32)
        places.append((ids[:, k : k + 1] ^ where_ref[0], rank_k))

    def hits_of(group):
        slots = lax.broadcasted_iota(jnp.int32, (token_count, len(group) * capacity), 1)
        out = []
        for block, rank_k in places:
            place = jnp.full_like(rank_k, -1)
            for at, k in enumerate(group):
                place = jnp.where(block == k, at * capacity + rank_k, place)
            out.append(jnp.where(place == slots, 1.0, 0.0).astype(jnp.bfloat16))
        return jnp.concatenate(out, axis=0)

    early = [k for group in members[:-1] for k in group]
    hits_ref[...] = hits_of(members[-1])
    hits = hits_of(early)
    for tile in tiles(sum_ref.shape[1]):
        sum_ref[:, tile] = mix(hits, gates, row_refs, tile, picks)


def finish_kernel(picks, where_ref, sum_ref, hits_ref, columns_ref, *refs):
    row_refs, out_ref = refs[:-1], refs[-1]
    gates = columns_ref[:, picks : 2 * picks]
    for tile in tiles(out_ref.shape[1]):
        total = sum_ref[:, tile] + mix(hits_ref[...], gates, row_refs, tile, picks)
        out_ref[:, tile] = total.astype(out_ref.dtype)


def combine(returned, members, ids, gates, where):
    capacity, width = returned[0].shape
    picks, token_count = ids.shape
    early = [returned[k] for group in members[:-1] for k in group]
    late = [returned[k] for k in members[-1]]
    block = whole_spec((capacity, width))
    outs = [
        jax.ShapeDtypeStruct((token_count, width), jnp.float32),
        jax.ShapeDtypeStruct((picks * token_count, len(late) * capacity), returned[0].dtype),
        jax.ShapeDtypeStruct((token_count, 2 * picks + (-2 * picks % 8)), jnp.float32),
    ]
    flops = 2 * picks * capacity * token_count * width
    begun = call(
        functools.partial(begin_kernel, members), (1,), [ids, gates, *early],
        [whole_spec(ids.shape), whole_spec(gates.shape)] + [block] * len(early),
        outs, [whole_spec(out.shape) for out in outs], flops * len(early), where,
    )
    out = jax.ShapeDtypeStruct((token_count, width), returned[0].dtype)
    return call(
        functools.partial(finish_kernel, picks), (1,), [*begun, *late],
        [whole_spec(x.shape) for x in outs] + [block] * len(late),
        out, whole_spec(out.shape), flops * len(late), where,
    )


def block_positions(starts_ref, owner, count, axis):
    shape = (count, 1) if axis == 0 else (1, count)
    index = lax.broadcasted_iota(jnp.int32, shape, axis)
    half = count // 2
    first, second = starts_ref[2 * owner], starts_ref[2 * owner + 1]
    return jnp.where(index < half, first + index, second + index - half)


def attention_kernel(where_ref, starts_ref, queries_ref, uv_ref, *refs):
    keys, out_ref, flipped, joined, late = refs[:-4], refs[-4], refs[-3], refs[-2], refs[-1]
    token_count = queries_ref.shape[2]
    lat_width = uv_ref.shape[1]
    query_positions = block_positions(starts_ref, where_ref[1], token_count, 1)
    for j, block in enumerate(keys):
        at = slice(j * token_count, (j + 1) * token_count)
        flipped[:, at] = block[...]
        joined[at, :] = block[...].T
        key_positions = block_positions(starts_ref, where_ref[1] ^ j, token_count, 0)
        late[at, :] = jnp.where(key_positions <= query_positions, 0.0, neg_fill)

    @pl.loop(0, queries_ref.shape[0])
    def _(head):
        scores = jnp.dot(joined[...], queries_ref[head], preferred_element_type=jnp.float32)
        hidden = late[...] < 0.0
        masked = jnp.where(hidden, neg_fill, scores * score_scale)
        top_score = jnp.max(masked, axis=0, keepdims=True)
        weights = jnp.where(hidden, 0.0, jnp.exp(masked - top_score))
        totals = jnp.sum(weights, axis=0, keepdims=True)
        blended = jnp.dot(
            flipped[:lat_width, :], weights.astype(jnp.bfloat16), preferred_element_type=jnp.float32
        )
        latent_out = (blended / totals).astype(jnp.bfloat16)
        out_ref[head] = lax.dot_general(
            latent_out, uv_ref[head], (((0,), (0,)), ((), ())), preferred_element_type=jnp.float32
        ).astype(out_ref.dtype)


def attention(queries, keys, block_starts, w_uv, where):
    head_count, entry_width, token_count = queries.shape
    key_count = len(keys) * token_count
    shape = (head_count, token_count, w_uv.shape[2])
    return call(
        attention_kernel, (1,), [queries, w_uv, *keys],
        [whole_spec(queries.shape), whole_spec(w_uv.shape)]
        + [whole_spec((entry_width, token_count))] * len(keys),
        jax.ShapeDtypeStruct(shape, queries.dtype), whole_spec(shape),
        4 * head_count * key_count * token_count * entry_width, (where, block_starts),
        vmem=24 << 20,
        scratch=[
            pltpu.VMEM((entry_width, key_count), queries.dtype),
            pltpu.VMEM((key_count, entry_width), queries.dtype),
            pltpu.VMEM((key_count, token_count), jnp.float32),
        ],
    )


def layer(
    queries, latents, block_starts, w_uv, moe_tokens, expert_ids, gate_weights, w_gate, w_up, w_down
):
    token_count, picks = expert_ids.shape
    expert_count = lax.axis_size("exp")
    ctx_size = lax.axis_size("ctx")
    width = moe_tokens.shape[1] // ctx_size
    capacity = 3 * token_count * picks // (2 * expert_count)
    where = where_am_i()
    evens = range(2, ctx_size, 2)

    slices = split_columns(w_down[0], width, where)
    down_parts = [swap(slices[offset - 1], "ctx", offset) for offset in range(1, ctx_size)]

    outgoing = dispatch(moe_tokens, expert_ids.T, capacity, expert_count, width, where)
    sets = set_members(expert_count)
    arrived = [swap(outgoing[k], "exp", k) if k else outgoing[0] for k in range(expert_count)]

    returned = [None] * expert_count
    for s, members in enumerate(sets):
        chunks = pack([arrived[k] for k in members], CHUNKS[s], where)
        pieces = [None] * ctx_size
        pieces[0] = chunks
        for offset in evens:
            pieces[offset] = [swap(chunk, "ctx", offset) for chunk in chunks]
        for offset in range(0, ctx_size, 2):
            pieces[offset + 1] = [swap(chunk, "ctx", 1) for chunk in pieces[offset]]
        partial = mlp(pieces[:2], [0, 1], w_gate[0], w_up[0], None, where)
        hidden = mlp(pieces[2:], range(2, ctx_size), w_gate[0], w_up[0], partial, where)
        hidden = [hidden] + [swap(hidden, "ctx", offset) for offset in range(1, ctx_size)]
        blocks = down(hidden, w_down[0], down_parts, len(members), where)
        for k, block in zip(members, blocks):
            returned[k] = swap(block, "exp", k) if k else block

    keys = [latents.T] + [None] * (ctx_size - 1)
    for offset in evens:
        keys[offset] = swap(keys[0], "ctx", offset)
    for offset in range(0, ctx_size, 2):
        keys[offset + 1] = swap(keys[offset], "ctx", 1)
    attended = attention(jnp.transpose(queries, (1, 2, 0)), keys, block_starts, w_uv, where)
    attended = jnp.transpose(attended, (1, 0, 2))
    return attended, combine(returned, sets, expert_ids.T, gate_weights.T, where)


def solution(mesh):
    in_specs = (
        P("ctx", "exp", None),
        P("ctx", None),
        P(),
        P("exp", None, None),
        P("exp", None),
        P("exp", None),
        P("exp", None),
        P("exp", None, "ctx"),
        P("exp", None, "ctx"),
        P("exp", "ctx", None),
    )
    out_specs = (P("ctx", "exp", None), P("exp", "ctx"))
    return jax.shard_map(layer, mesh=mesh, in_specs=in_specs, out_specs=out_specs, check_vma=False)
```

```python
import functools
import math

import jax
import jax.numpy as jnp
from jax import lax
from jax.experimental import pallas as pl
from jax.experimental.pallas import tpu as pltpu
from jax.sharding import PartitionSpec as P


score_scale = (0.1 * math.log(40.0) + 1.0) ** 2 / math.sqrt(192.0)
neg_fill = -1e30


def swap(x, axis, offset):
    size = lax.axis_size(axis)
    return lax.ppermute(x, axis, [(i, i ^ offset) for i in range(size)])


def set_members(expert_count):
    cut = expert_count - expert_count // 4
    return [list(range(cut, expert_count)), list(range(cut))]


def is_doubled(ctx_size, width):
    return ctx_size == 4 and width % 256 == 0


def where_am_i():
    return jnp.stack([lax.axis_index("exp"), lax.axis_index("ctx")]).astype(jnp.int32)


def whole_spec(shape):
    return pl.BlockSpec(shape, lambda i, *_: (0,) * len(shape))


def call(kernel, grid, operands, in_specs, out_shape, out_specs, flops, scalars, vmem=16 << 20, scratch=()):
    scalars = scalars if isinstance(scalars, tuple) else (scalars,)
    shapes = jax.tree.leaves(out_shape)
    moved = sum(math.prod(x.shape) * x.dtype.itemsize for x in list(operands) + shapes)
    return pl.pallas_call(
        kernel,
        out_shape=out_shape,
        grid_spec=pltpu.PrefetchScalarGridSpec(
            num_scalar_prefetch=len(scalars), grid=grid, in_specs=in_specs, out_specs=out_specs,
            scratch_shapes=scratch,
        ),
        cost_estimate=pl.CostEstimate(flops=flops, bytes_accessed=moved, transcendentals=0),
        compiler_params=pltpu.CompilerParams(vmem_limit_bytes=vmem),
    )(*scalars, *operands)


def split_kernel(where_ref, *refs):
    half = len(refs) // 2
    for source, target in zip(refs[:half], refs[half:]):
        target[...] = source[...]


def split_columns(matrix, width, where):
    rows, ctx_size = matrix.shape[0], matrix.shape[1] // width
    count = ctx_size - 1
    operands = [matrix] * count
    specs = [
        pl.BlockSpec((rows, width), lambda i, w, k=k: (0, w[1] ^ k)) for k in range(1, ctx_size)
    ]
    if width % 128:
        specs = [whole_spec((rows, width))] * count
        operands = [
            lax.dynamic_slice_in_dim(matrix, (where[1] ^ k) * width, width, axis=1)
            for k in range(1, ctx_size)
        ]
    out = jax.ShapeDtypeStruct((rows, width), matrix.dtype)
    return call(
        split_kernel, (1,), operands, specs,
        [out] * count, [whole_spec((rows, width))] * count, rows * width, where,
    )


def own_columns(matrix, width, where):
    rows = matrix.shape[0]
    if width % 128:
        return lax.dynamic_slice_in_dim(matrix, where[1] * width, width, axis=1), whole_spec((rows, width))
    return matrix, pl.BlockSpec((rows, width), lambda i, w: (0, w[1]))


def dispatch_kernel(capacity, expert_count, members, where_ref, ids_ref, *refs):
    ids = ids_ref[...]
    picks, token_count = ids.shape
    experts = lax.broadcasted_iota(jnp.int32, (expert_count, token_count), 0)
    named = jnp.zeros((expert_count, token_count), jnp.float32)
    for k in range(picks):
        named = named + jnp.where(ids[k : k + 1, :] == experts, 1.0, 0.0)
    rows = lax.broadcasted_iota(jnp.int32, (token_count, token_count), 0)
    cols = lax.broadcasted_iota(jnp.int32, (token_count, token_count), 1)
    before = jnp.where(rows < cols, 1.0, 0.0).astype(jnp.bfloat16)
    rank = jnp.dot(named.astype(jnp.bfloat16), before, preferred_element_type=jnp.float32)
    slots = lax.broadcasted_iota(jnp.int32, (expert_count * capacity, token_count), 0)
    chosen = None
    for k in range(picks):
        own = jnp.where(ids[k : k + 1, :] == experts, rank, 0.0)
        place = jnp.sum(own, axis=0, keepdims=True).astype(jnp.int32)
        place = place + (ids[k : k + 1, :] ^ where_ref[0]) * capacity
        hit = jnp.where(place == slots, 1.0, 0.0)
        chosen = hit if chosen is None else chosen + hit
    chosen = chosen.astype(jnp.bfloat16)
    sources = refs[: 2 if members else 1]
    targets = refs[len(sources) :]
    own, half = sources[0], sources[0].shape[1] // 2

    def send(group, columns, outs, at):
        pick = jnp.concatenate(
            [chosen[k * capacity : (k + 1) * capacity, :] for k in group], axis=0
        )
        rows = jnp.dot(pick, columns, preferred_element_type=jnp.float32).astype(own.dtype)
        for n, out in enumerate(outs):
            out[:, at : at + rows.shape[1]] = rows[n * capacity : (n + 1) * capacity, :]

    whole = [k for k in range(expert_count) if k not in members]
    send(whole, own[...], targets[: len(whole)], 0)
    if members:
        late = targets[len(whole) : len(whole) + len(members)]
        first = targets[len(whole) + len(members) :]
        send(members, own[:, half:], late, 0)
        send(members, own[:, :half], first, 0)
        send(members, sources[1][...], first, half)


def dispatch(tokens, ids, capacity, expert_count, width, members, where):
    token_count = tokens.shape[0]
    operand, spec = own_columns(tokens, width, where)
    operands, specs = [operand], [spec]
    if members:
        operands.append(tokens)
        specs.append(pl.BlockSpec((token_count, width // 2), lambda i, w: (0, (w[1] ^ 2) * 2)))
    widths = [width] * (expert_count - len(members)) + [width // 2] * len(members)
    widths += [width] * len(members)
    blocks = [(capacity, w) for w in widths]
    outs = call(
        functools.partial(dispatch_kernel, capacity, expert_count, members), (1,),
        [ids, *operands], [whole_spec(ids.shape), *specs],
        [jax.ShapeDtypeStruct(block, tokens.dtype) for block in blocks],
        [whole_spec(block) for block in blocks],
        2 * expert_count * capacity * token_count * width, where,
    )
    order = [k for k in range(expert_count) if k not in members] + members
    first = dict(zip(members, outs[expert_count:]))
    return dict(zip(order, outs)), first


def pack_kernel(where_ref, *refs):
    rows = refs[0].shape[0]
    for i, source in enumerate(refs[:-1]):
        refs[-1][i * rows : (i + 1) * rows, :] = source[...]


def pack(blocks, where):
    rows, width = blocks[0].shape
    shape = (len(blocks) * rows, width)
    return call(
        pack_kernel, (1,), blocks, [whole_spec((rows, width))] * len(blocks),
        jax.ShapeDtypeStruct(shape, blocks[0].dtype), whole_spec(shape), shape[0] * width, where,
    )


def up_sum(count, refs):
    acc = None
    for j in range(count):
        weights = jnp.concatenate([refs[j][...], refs[count + j][...]], axis=1)
        term = jnp.dot(refs[2 * count + j][...], weights, preferred_element_type=jnp.float32)
        acc = term if acc is None else acc + term
    return acc


def part_kernel(count, where_ref, *refs):
    refs[-1][...] = up_sum(count, refs[:-1])


def mlp_kernel(count, where_ref, *refs):
    acc = refs[-2][...] + up_sum(count, refs[:-2])
    hidden_width = acc.shape[1] // 2
    gate_h, up_h = acc[:, :hidden_width], acc[:, hidden_width:]
    refs[-1][...] = (gate_h / (1.0 + jnp.exp(-gate_h)) * up_h).astype(refs[-1].dtype)


def mlp(pieces, width, gate_matrix, up_matrix, partial, where):
    count, hidden_width = len(pieces), gate_matrix.shape[1]
    rows = pieces[0][0].shape[0]
    arrays = [piece[0] for piece in pieces]
    specs = [
        pl.BlockSpec((w, hidden_width), lambda i, m, k=k, n=width // w, b=b: ((m[1] ^ k) * n + b, 0))
        for x, at, k, b, w in pieces
    ]
    row_specs = [
        whole_spec(x.shape) if x.shape[1] == w else pl.BlockSpec((rows, w), lambda i, m, at=at: (0, at))
        for x, at, k, b, w in pieces
    ]
    operands = [gate_matrix] * count + [up_matrix] * count + arrays
    specs = specs + specs + row_specs
    if partial is None:
        kernel, out = part_kernel, jax.ShapeDtypeStruct((rows, 2 * hidden_width), jnp.float32)
    else:
        kernel, out = mlp_kernel, jax.ShapeDtypeStruct((rows, hidden_width), arrays[0].dtype)
        operands.append(partial)
        specs.append(whole_spec(partial.shape))
    columns = sum(piece[4] for piece in pieces)
    return call(
        functools.partial(kernel, count), (1,), operands, specs, out, whole_spec(out.shape),
        4 * rows * columns * hidden_width, where, vmem=24 << 20,
    )


def tiles(width):
    step = 256 if width % 256 == 0 else width
    return [slice(at, at + step) for at in range(0, width, step)]


def down_kernel(count, where_ref, *refs):
    parts, out_refs = refs[count : 2 * count], refs[2 * count :]
    rows, width = out_refs[0].shape
    hidden = jnp.concatenate([ref[...] for ref in refs[:count]], axis=1)
    for tile in tiles(width):
        matrix = jnp.concatenate([part[:, tile] for part in parts], axis=0)
        out = jnp.dot(hidden, matrix, preferred_element_type=jnp.float32)
        out = out.astype(out_refs[0].dtype)
        for i, target in enumerate(out_refs):
            target[:, tile] = out[i * rows : (i + 1) * rows, :]


def down(hidden, own, others, block_count, where):
    width, count = others[0].shape[1], len(hidden)
    operand, spec = own_columns(own, width, where)
    block = (hidden[0].shape[0] // block_count, width)
    return call(
        functools.partial(down_kernel, count), (1,), [*hidden, operand, *others],
        [whole_spec(hidden[0].shape)] * count + [spec] + [whole_spec(others[0].shape)] * len(others),
        [jax.ShapeDtypeStruct(block, hidden[0].dtype)] * block_count,
        [whole_spec(block)] * block_count,
        2 * count * math.prod(hidden[0].shape) * width, where,
    )


def mix(hits, gates, row_refs, tile, picks):
    token_count = hits.shape[0] // picks
    arrived = jnp.concatenate([ref[:, tile] for ref in row_refs], axis=0)
    chosen = jnp.dot(hits, arrived, preferred_element_type=jnp.float32)
    total = None
    for k in range(picks):
        term = chosen[k * token_count : (k + 1) * token_count, :] * gates[:, k : k + 1]
        total = term if total is None else total + term
    return total


def begin_kernel(members, where_ref, ids_ref, gates_ref, *refs):
    row_refs, sum_ref, hits_ref, columns_ref = refs[:-3], refs[-3], refs[-2], refs[-1]
    expert_count, capacity = sum(len(m) for m in members), row_refs[0].shape[0]
    picks, token_count = ids_ref.shape
    columns = jnp.concatenate(
        [ids_ref[...].astype(jnp.float32), gates_ref[...]]
        + [jnp.zeros((-2 * picks % 8, token_count), jnp.float32)],
        axis=0,
    ).T
    columns_ref[...] = columns
    ids, gates = columns[:, :picks].astype(jnp.int32), columns[:, picks : 2 * picks]
    experts = lax.broadcasted_iota(jnp.int32, (token_count, expert_count), 1)
    named = jnp.zeros((token_count, expert_count), jnp.float32)
    for k in range(picks):
        named = named + jnp.where(ids[:, k : k + 1] == experts, 1.0, 0.0)
    rows = lax.broadcasted_iota(jnp.int32, (token_count, token_count), 0)
    cols = lax.broadcasted_iota(jnp.int32, (token_count, token_count), 1)
    before = jnp.where(cols < rows, 1.0, 0.0).astype(jnp.bfloat16)
    rank = jnp.dot(before, named.astype(jnp.bfloat16), preferred_element_type=jnp.float32)
    places = []
    for k in range(picks):
        own = jnp.where(ids[:, k : k + 1] == experts, rank, 0.0)
        rank_k = jnp.sum(own, axis=1, keepdims=True).astype(jnp.int32)
        places.append((ids[:, k : k + 1] ^ where_ref[0], rank_k))

    def hits_of(group):
        slots = lax.broadcasted_iota(jnp.int32, (token_count, len(group) * capacity), 1)
        out = []
        for block, rank_k in places:
            place = jnp.full_like(rank_k, -1)
            for at, k in enumerate(group):
                place = jnp.where(block == k, at * capacity + rank_k, place)
            out.append(jnp.where(place == slots, 1.0, 0.0).astype(jnp.bfloat16))
        return jnp.concatenate(out, axis=0)

    early = [k for group in members[:-1] for k in group]
    hits_ref[...] = hits_of(members[-1])
    hits = hits_of(early)
    for tile in tiles(sum_ref.shape[1]):
        sum_ref[:, tile] = mix(hits, gates, row_refs, tile, picks)


def finish_kernel(picks, where_ref, sum_ref, hits_ref, columns_ref, *refs):
    row_refs, out_ref = refs[:-1], refs[-1]
    gates = columns_ref[:, picks : 2 * picks]
    for tile in tiles(out_ref.shape[1]):
        total = sum_ref[:, tile] + mix(hits_ref[...], gates, row_refs, tile, picks)
        out_ref[:, tile] = total.astype(out_ref.dtype)


def combine(returned, members, ids, gates, where):
    capacity, width = returned[0].shape
    picks, token_count = ids.shape
    early = [returned[k] for group in members[:-1] for k in group]
    late = [returned[k] for k in members[-1]]
    block = whole_spec((capacity, width))
    outs = [
        jax.ShapeDtypeStruct((token_count, width), jnp.float32),
        jax.ShapeDtypeStruct((picks * token_count, len(late) * capacity), returned[0].dtype),
        jax.ShapeDtypeStruct((token_count, 2 * picks + (-2 * picks % 8)), jnp.float32),
    ]
    flops = 2 * picks * capacity * token_count * width
    begun = call(
        functools.partial(begin_kernel, members), (1,), [ids, gates, *early],
        [whole_spec(ids.shape), whole_spec(gates.shape)] + [block] * len(early),
        outs, [whole_spec(out.shape) for out in outs], flops * len(early), where,
    )
    out = jax.ShapeDtypeStruct((token_count, width), returned[0].dtype)
    return call(
        functools.partial(finish_kernel, picks), (1,), [*begun, *late],
        [whole_spec(x.shape) for x in outs] + [block] * len(late),
        out, whole_spec(out.shape), flops * len(late), where,
    )


def block_positions(starts_ref, owner, count, axis):
    shape = (count, 1) if axis == 0 else (1, count)
    index = lax.broadcasted_iota(jnp.int32, shape, axis)
    half = count // 2
    first, second = starts_ref[2 * owner], starts_ref[2 * owner + 1]
    return jnp.where(index < half, first + index, second + index - half)


def attention_kernel(where_ref, starts_ref, queries_ref, uv_ref, *refs):
    keys, out_ref, flipped, joined, late = refs[:-4], refs[-4], refs[-3], refs[-2], refs[-1]
    token_count = queries_ref.shape[2]
    lat_width = uv_ref.shape[1]
    query_positions = block_positions(starts_ref, where_ref[1], token_count, 1)
    for j, block in enumerate(keys):
        at = slice(j * token_count, (j + 1) * token_count)
        flipped[:, at] = block[...]
        joined[at, :] = block[...].T
        key_positions = block_positions(starts_ref, where_ref[1] ^ j, token_count, 0)
        late[at, :] = jnp.where(key_positions <= query_positions, 0.0, neg_fill)

    @pl.loop(0, queries_ref.shape[0])
    def _(head):
        scores = jnp.dot(joined[...], queries_ref[head], preferred_element_type=jnp.float32)
        hidden = late[...] < 0.0
        masked = jnp.where(hidden, neg_fill, scores * score_scale)
        top_score = jnp.max(masked, axis=0, keepdims=True)
        weights = jnp.where(hidden, 0.0, jnp.exp(masked - top_score))
        totals = jnp.sum(weights, axis=0, keepdims=True)
        blended = jnp.dot(
            flipped[:lat_width, :], weights.astype(jnp.bfloat16), preferred_element_type=jnp.float32
        )
        latent_out = (blended / totals).astype(jnp.bfloat16)
        out_ref[head] = lax.dot_general(
            latent_out, uv_ref[head], (((0,), (0,)), ((), ())), preferred_element_type=jnp.float32
        ).astype(out_ref.dtype)


def attention(queries, keys, block_starts, w_uv, where):
    head_count, entry_width, token_count = queries.shape
    key_count = len(keys) * token_count
    shape = (head_count, token_count, w_uv.shape[2])
    return call(
        attention_kernel, (1,), [queries, w_uv, *keys],
        [whole_spec(queries.shape), whole_spec(w_uv.shape)]
        + [whole_spec((entry_width, token_count))] * len(keys),
        jax.ShapeDtypeStruct(shape, queries.dtype), whole_spec(shape),
        4 * head_count * key_count * token_count * entry_width, (where, block_starts),
        vmem=24 << 20,
        scratch=[
            pltpu.VMEM((entry_width, key_count), queries.dtype),
            pltpu.VMEM((key_count, entry_width), queries.dtype),
            pltpu.VMEM((key_count, token_count), jnp.float32),
        ],
    )


def layer(
    queries, latents, block_starts, w_uv, moe_tokens, expert_ids, gate_weights, w_gate, w_up, w_down
):
    token_count, picks = expert_ids.shape
    expert_count = lax.axis_size("exp")
    ctx_size = lax.axis_size("ctx")
    width = moe_tokens.shape[1] // ctx_size
    capacity = 3 * token_count * picks // (2 * expert_count)
    where = where_am_i()
    evens = range(2, ctx_size, 2)

    slices = split_columns(w_down[0], width, where)
    down_parts = [swap(slices[offset - 1], "ctx", offset) for offset in range(1, ctx_size)]

    sets = set_members(expert_count)
    doubled = sets[-1] if is_doubled(ctx_size, width) else []
    outgoing, first = dispatch(
        moe_tokens, expert_ids.T, capacity, expert_count, width, doubled, where
    )
    arrived = [swap(outgoing[k], "exp", k) if k else outgoing[0] for k in range(expert_count)]

    returned = [None] * expert_count
    for members in sets:
        own = pack([arrived[k] for k in members], where)
        beside = swap(own, "ctx", 1)
        w, b = own.shape[1], width // own.shape[1] - 1
        early = [(own, 0, 0, b, w), (beside, 0, 1, b, w)]
        late = []
        for offset in evens:
            crossed = swap(own, "ctx", offset)
            late += [(crossed, 0, offset, b, w)]
            late += [(swap(crossed, "ctx", 1), 0, offset + 1, b, w)]
        if w != width:
            both = [swap(first[k], "exp", k) if k else first[k] for k in members]
            both = pack(both, where)
            other = swap(both, "ctx", 1)
            early += [(both, 0, 0, 0, w), (both, 1, 2, 0, w), (other, 0, 1, 0, w), (other, 1, 3, 0, w)]
        partial = mlp(early, width, w_gate[0], w_up[0], None, where)
        hidden = mlp(late, width, w_gate[0], w_up[0], partial, where)
        hidden = [hidden] + [swap(hidden, "ctx", offset) for offset in range(1, ctx_size)]
        blocks = down(hidden, w_down[0], down_parts, len(members), where)
        for k, block in zip(members, blocks):
            returned[k] = swap(block, "exp", k) if k else block

    keys = [latents.T] + [None] * (ctx_size - 1)
    for offset in evens:
        keys[offset] = swap(keys[0], "ctx", offset)
    for offset in range(0, ctx_size, 2):
        keys[offset + 1] = swap(keys[offset], "ctx", 1)
    attended = attention(jnp.transpose(queries, (1, 2, 0)), keys, block_starts, w_uv, where)
    attended = jnp.transpose(attended, (1, 0, 2))
    return attended, combine(returned, sets, expert_ids.T, gate_weights.T, where)


def solution(mesh):
    in_specs = (
        P("ctx", "exp", None),
        P("ctx", None),
        P(),
        P("exp", None, None),
        P("exp", None),
        P("exp", None),
        P("exp", None),
        P("exp", None, "ctx"),
        P("exp", None, "ctx"),
        P("exp", "ctx", None),
    )
    out_specs = (P("ctx", "exp", None), P("exp", "ctx"))
    return jax.shard_map(layer, mesh=mesh, in_specs=in_specs, out_specs=out_specs, check_vma=False)
```

```python
import functools
import math

import jax
import jax.numpy as jnp
from jax import lax
from jax.experimental import pallas as pl
from jax.experimental.pallas import tpu as pltpu
from jax.sharding import PartitionSpec as P


score_scale = (0.1 * math.log(40.0) + 1.0) ** 2 / math.sqrt(192.0)
neg_fill = -1e30


def swap(x, axis, offset):
    size = lax.axis_size(axis)
    return lax.ppermute(x, axis, [(i, i ^ offset) for i in range(size)])


def set_members(expert_count):
    half, cut = expert_count // 2, expert_count - expert_count // 4
    return [list(range(cut, expert_count)), list(range(half, cut)), list(range(half))]


def is_doubled(ctx_size, width):
    return ctx_size == 4 and width % 128 == 0


def where_am_i():
    return jnp.stack([lax.axis_index("exp"), lax.axis_index("ctx")]).astype(jnp.int32)


def whole_spec(shape):
    return pl.BlockSpec(shape, lambda i, *_: (0,) * len(shape))


def call(kernel, grid, operands, in_specs, out_shape, out_specs, flops, scalars, vmem=16 << 20, scratch=()):
    scalars = scalars if isinstance(scalars, tuple) else (scalars,)
    shapes = jax.tree.leaves(out_shape)
    moved = sum(math.prod(x.shape) * x.dtype.itemsize for x in list(operands) + shapes)
    return pl.pallas_call(
        kernel,
        out_shape=out_shape,
        grid_spec=pltpu.PrefetchScalarGridSpec(
            num_scalar_prefetch=len(scalars), grid=grid, in_specs=in_specs, out_specs=out_specs,
            scratch_shapes=scratch,
        ),
        cost_estimate=pl.CostEstimate(flops=flops, bytes_accessed=moved, transcendentals=0),
        compiler_params=pltpu.CompilerParams(vmem_limit_bytes=vmem),
    )(*scalars, *operands)


def split_kernel(where_ref, *refs):
    half = len(refs) // 2
    for source, target in zip(refs[:half], refs[half:]):
        target[...] = source[...]


def split_columns(matrix, width, where):
    rows, ctx_size = matrix.shape[0], matrix.shape[1] // width
    count = ctx_size - 1
    operands = [matrix] * count
    specs = [
        pl.BlockSpec((rows, width), lambda i, w, k=k: (0, w[1] ^ k)) for k in range(1, ctx_size)
    ]
    if width % 128:
        specs = [whole_spec((rows, width))] * count
        operands = [
            lax.dynamic_slice_in_dim(matrix, (where[1] ^ k) * width, width, axis=1)
            for k in range(1, ctx_size)
        ]
    out = jax.ShapeDtypeStruct((rows, width), matrix.dtype)
    return call(
        split_kernel, (1,), operands, specs,
        [out] * count, [whole_spec((rows, width))] * count, rows * width, where,
    )


def own_columns(matrix, width, where):
    rows = matrix.shape[0]
    if width % 128:
        return lax.dynamic_slice_in_dim(matrix, where[1] * width, width, axis=1), whole_spec((rows, width))
    return matrix, pl.BlockSpec((rows, width), lambda i, w: (0, w[1]))


def dispatch_kernel(capacity, expert_count, members, where_ref, ids_ref, *refs):
    ids = ids_ref[...]
    picks, token_count = ids.shape
    experts = lax.broadcasted_iota(jnp.int32, (expert_count, token_count), 0)
    named = jnp.zeros((expert_count, token_count), jnp.float32)
    for k in range(picks):
        named = named + jnp.where(ids[k : k + 1, :] == experts, 1.0, 0.0)
    rows = lax.broadcasted_iota(jnp.int32, (token_count, token_count), 0)
    cols = lax.broadcasted_iota(jnp.int32, (token_count, token_count), 1)
    before = jnp.where(rows < cols, 1.0, 0.0).astype(jnp.bfloat16)
    rank = jnp.dot(named.astype(jnp.bfloat16), before, preferred_element_type=jnp.float32)
    slots = lax.broadcasted_iota(jnp.int32, (expert_count * capacity, token_count), 0)
    chosen = None
    for k in range(picks):
        own = jnp.where(ids[k : k + 1, :] == experts, rank, 0.0)
        place = jnp.sum(own, axis=0, keepdims=True).astype(jnp.int32)
        place = place + (ids[k : k + 1, :] ^ where_ref[0]) * capacity
        hit = jnp.where(place == slots, 1.0, 0.0)
        chosen = hit if chosen is None else chosen + hit
    chosen = chosen.astype(jnp.bfloat16)
    sources = refs[: 2 if members else 1]
    targets = refs[len(sources) :]
    width = sources[0].shape[1]
    for n, source in enumerate(sources):
        group = members if n else range(expert_count)
        pick = chosen
        if n:
            pick = jnp.concatenate(
                [chosen[k * capacity : (k + 1) * capacity, :] for k in group], axis=0
            )
        rows = jnp.dot(pick, source[...], preferred_element_type=jnp.float32).astype(source.dtype)
        for at, k in enumerate(group):
            targets[k][:, n * width : (n + 1) * width] = rows[at * capacity : (at + 1) * capacity, :]


def dispatch(tokens, ids, capacity, expert_count, width, members, where):
    operand, spec = own_columns(tokens, width, where)
    operands, specs = [operand], [spec]
    if members:
        operands.append(tokens)
        specs.append(pl.BlockSpec((tokens.shape[0], width), lambda i, w: (0, w[1] ^ 2)))
    blocks = [(capacity, 2 * width if k in members else width) for k in range(expert_count)]
    return call(
        functools.partial(dispatch_kernel, capacity, expert_count, members), (1,),
        [ids, *operands], [whole_spec(ids.shape), *specs],
        [jax.ShapeDtypeStruct(block, tokens.dtype) for block in blocks],
        [whole_spec(block) for block in blocks],
        2 * expert_count * capacity * tokens.shape[0] * width, where,
    )


def pack_kernel(where_ref, *refs):
    rows = refs[0].shape[0]
    for i, source in enumerate(refs[:-1]):
        refs[-1][i * rows : (i + 1) * rows, :] = source[...]


def pack(blocks, where):
    rows, width = blocks[0].shape
    shape = (len(blocks) * rows, width)
    return call(
        pack_kernel, (1,), blocks, [whole_spec((rows, width))] * len(blocks),
        jax.ShapeDtypeStruct(shape, blocks[0].dtype), whole_spec(shape), shape[0] * width, where,
    )


def up_sum(count, refs):
    acc = None
    for j in range(count):
        weights = jnp.concatenate([refs[j][...], refs[count + j][...]], axis=1)
        term = jnp.dot(refs[2 * count + j][...], weights, preferred_element_type=jnp.float32)
        acc = term if acc is None else acc + term
    return acc


def part_kernel(count, where_ref, *refs):
    refs[-1][...] = up_sum(count, refs[:-1])


def mlp_kernel(count, where_ref, *refs):
    acc = refs[-2][...] + up_sum(count, refs[:-2])
    hidden_width = acc.shape[1] // 2
    gate_h, up_h = acc[:, :hidden_width], acc[:, hidden_width:]
    refs[-1][...] = (gate_h / (1.0 + jnp.exp(-gate_h)) * up_h).astype(refs[-1].dtype)


def mlp(pieces, width, gate_matrix, up_matrix, partial, where):
    count, hidden_width = len(pieces), gate_matrix.shape[1]
    rows = pieces[0][0].shape[0]
    arrays = [piece[0] for piece in pieces]
    specs = [
        pl.BlockSpec((width, hidden_width), lambda i, m, k=k: (m[1] ^ k, 0)) for x, at, k in pieces
    ]
    row_specs = [
        whole_spec(x.shape)
        if x.shape[1] == width
        else pl.BlockSpec((rows, width), lambda i, m, at=at: (0, at))
        for x, at, k in pieces
    ]
    operands = [gate_matrix] * count + [up_matrix] * count + arrays
    specs = specs + specs + row_specs
    if partial is None:
        kernel, out = part_kernel, jax.ShapeDtypeStruct((rows, 2 * hidden_width), jnp.float32)
    else:
        kernel, out = mlp_kernel, jax.ShapeDtypeStruct((rows, hidden_width), arrays[0].dtype)
        operands.append(partial)
        specs.append(whole_spec(partial.shape))
    columns = count * width
    return call(
        functools.partial(kernel, count), (1,), operands, specs, out, whole_spec(out.shape),
        4 * rows * columns * hidden_width, where, vmem=24 << 20,
    )


def tiles(width):
    step = 256 if width % 256 == 0 else width
    return [slice(at, at + step) for at in range(0, width, step)]


def down_kernel(count, where_ref, *refs):
    parts, out_refs = refs[count : 2 * count], refs[2 * count :]
    rows, width = out_refs[0].shape
    hidden = jnp.concatenate([ref[...] for ref in refs[:count]], axis=1)
    for tile in tiles(width):
        matrix = jnp.concatenate([part[:, tile] for part in parts], axis=0)
        out = jnp.dot(hidden, matrix, preferred_element_type=jnp.float32)
        out = out.astype(out_refs[0].dtype)
        for i, target in enumerate(out_refs):
            target[:, tile] = out[i * rows : (i + 1) * rows, :]


def down(hidden, own, others, block_count, where):
    width, count = others[0].shape[1], len(hidden)
    operand, spec = own_columns(own, width, where)
    block = (hidden[0].shape[0] // block_count, width)
    return call(
        functools.partial(down_kernel, count), (1,), [*hidden, operand, *others],
        [whole_spec(hidden[0].shape)] * count + [spec] + [whole_spec(others[0].shape)] * len(others),
        [jax.ShapeDtypeStruct(block, hidden[0].dtype)] * block_count,
        [whole_spec(block)] * block_count,
        2 * count * math.prod(hidden[0].shape) * width, where,
    )


def mix(hits, gates, row_refs, tile, picks):
    token_count = hits.shape[0] // picks
    arrived = jnp.concatenate([ref[:, tile] for ref in row_refs], axis=0)
    chosen = jnp.dot(hits, arrived, preferred_element_type=jnp.float32)
    total = None
    for k in range(picks):
        term = chosen[k * token_count : (k + 1) * token_count, :] * gates[:, k : k + 1]
        total = term if total is None else total + term
    return total


def begin_kernel(members, where_ref, ids_ref, gates_ref, *refs):
    row_refs, sum_ref, hits_ref, columns_ref = refs[:-3], refs[-3], refs[-2], refs[-1]
    expert_count, capacity = sum(len(m) for m in members), row_refs[0].shape[0]
    picks, token_count = ids_ref.shape
    columns = jnp.concatenate(
        [ids_ref[...].astype(jnp.float32), gates_ref[...]]
        + [jnp.zeros((-2 * picks % 8, token_count), jnp.float32)],
        axis=0,
    ).T
    columns_ref[...] = columns
    ids, gates = columns[:, :picks].astype(jnp.int32), columns[:, picks : 2 * picks]
    experts = lax.broadcasted_iota(jnp.int32, (token_count, expert_count), 1)
    named = jnp.zeros((token_count, expert_count), jnp.float32)
    for k in range(picks):
        named = named + jnp.where(ids[:, k : k + 1] == experts, 1.0, 0.0)
    rows = lax.broadcasted_iota(jnp.int32, (token_count, token_count), 0)
    cols = lax.broadcasted_iota(jnp.int32, (token_count, token_count), 1)
    before = jnp.where(cols < rows, 1.0, 0.0).astype(jnp.bfloat16)
    rank = jnp.dot(before, named.astype(jnp.bfloat16), preferred_element_type=jnp.float32)
    places = []
    for k in range(picks):
        own = jnp.where(ids[:, k : k + 1] == experts, rank, 0.0)
        rank_k = jnp.sum(own, axis=1, keepdims=True).astype(jnp.int32)
        places.append((ids[:, k : k + 1] ^ where_ref[0], rank_k))

    def hits_of(group):
        slots = lax.broadcasted_iota(jnp.int32, (token_count, len(group) * capacity), 1)
        out = []
        for block, rank_k in places:
            place = jnp.full_like(rank_k, -1)
            for at, k in enumerate(group):
                place = jnp.where(block == k, at * capacity + rank_k, place)
            out.append(jnp.where(place == slots, 1.0, 0.0).astype(jnp.bfloat16))
        return jnp.concatenate(out, axis=0)

    early = [k for group in members[:-1] for k in group]
    hits_ref[...] = hits_of(members[-1])
    hits = hits_of(early)
    for tile in tiles(sum_ref.shape[1]):
        sum_ref[:, tile] = mix(hits, gates, row_refs, tile, picks)


def finish_kernel(picks, where_ref, sum_ref, hits_ref, columns_ref, *refs):
    row_refs, out_ref = refs[:-1], refs[-1]
    gates = columns_ref[:, picks : 2 * picks]
    for tile in tiles(out_ref.shape[1]):
        total = sum_ref[:, tile] + mix(hits_ref[...], gates, row_refs, tile, picks)
        out_ref[:, tile] = total.astype(out_ref.dtype)


def combine(returned, members, ids, gates, where):
    capacity, width = returned[0].shape
    picks, token_count = ids.shape
    early = [returned[k] for group in members[:-1] for k in group]
    late = [returned[k] for k in members[-1]]
    block = whole_spec((capacity, width))
    outs = [
        jax.ShapeDtypeStruct((token_count, width), jnp.float32),
        jax.ShapeDtypeStruct((picks * token_count, len(late) * capacity), returned[0].dtype),
        jax.ShapeDtypeStruct((token_count, 2 * picks + (-2 * picks % 8)), jnp.float32),
    ]
    flops = 2 * picks * capacity * token_count * width
    begun = call(
        functools.partial(begin_kernel, members), (1,), [ids, gates, *early],
        [whole_spec(ids.shape), whole_spec(gates.shape)] + [block] * len(early),
        outs, [whole_spec(out.shape) for out in outs], flops * len(early), where,
    )
    out = jax.ShapeDtypeStruct((token_count, width), returned[0].dtype)
    return call(
        functools.partial(finish_kernel, picks), (1,), [*begun, *late],
        [whole_spec(x.shape) for x in outs] + [block] * len(late),
        out, whole_spec(out.shape), flops * len(late), where,
    )


def block_positions(starts_ref, owner, count, axis):
    shape = (count, 1) if axis == 0 else (1, count)
    index = lax.broadcasted_iota(jnp.int32, shape, axis)
    half = count // 2
    first, second = starts_ref[2 * owner], starts_ref[2 * owner + 1]
    return jnp.where(index < half, first + index, second + index - half)


def attention_kernel(where_ref, starts_ref, queries_ref, uv_ref, *refs):
    keys, out_ref, flipped, joined, late = refs[:-4], refs[-4], refs[-3], refs[-2], refs[-1]
    token_count = queries_ref.shape[2]
    lat_width = uv_ref.shape[1]
    query_positions = block_positions(starts_ref, where_ref[1], token_count, 1)
    for j, block in enumerate(keys):
        at = slice(j * token_count, (j + 1) * token_count)
        flipped[:, at] = block[...]
        joined[at, :] = block[...].T
        key_positions = block_positions(starts_ref, where_ref[1] ^ j, token_count, 0)
        late[at, :] = jnp.where(key_positions <= query_positions, 0.0, neg_fill)

    head_count = queries_ref.shape[0]
    together = 2 if head_count % 2 == 0 else 1

    @pl.loop(0, head_count // together)
    def _(group):
        heads = [group * together + n for n in range(together)]
        rows = jnp.concatenate([queries_ref[head] for head in heads], axis=1)
        scores = jnp.dot(joined[...], rows, preferred_element_type=jnp.float32)
        hidden = jnp.concatenate([late[...]] * together, axis=1) < 0.0
        masked = jnp.where(hidden, neg_fill, scores * score_scale)
        top_score = jnp.max(masked, axis=0, keepdims=True)
        weights = jnp.where(hidden, 0.0, jnp.exp(masked - top_score))
        totals = jnp.sum(weights, axis=0, keepdims=True)
        blended = jnp.dot(
            flipped[:lat_width, :], weights.astype(jnp.bfloat16), preferred_element_type=jnp.float32
        )
        latent_out = (blended / totals).astype(jnp.bfloat16)
        for n, head in enumerate(heads):
            part = latent_out[:, n * token_count : (n + 1) * token_count]
            out_ref[head] = lax.dot_general(
                part, uv_ref[head], (((0,), (0,)), ((), ())), preferred_element_type=jnp.float32
            ).astype(out_ref.dtype)


def attention(queries, keys, block_starts, w_uv, where):
    head_count, entry_width, token_count = queries.shape
    key_count = len(keys) * token_count
    shape = (head_count, token_count, w_uv.shape[2])
    return call(
        attention_kernel, (1,), [queries, w_uv, *keys],
        [whole_spec(queries.shape), whole_spec(w_uv.shape)]
        + [whole_spec((entry_width, token_count))] * len(keys),
        jax.ShapeDtypeStruct(shape, queries.dtype), whole_spec(shape),
        4 * head_count * key_count * token_count * entry_width, (where, block_starts),
        vmem=24 << 20,
        scratch=[
            pltpu.VMEM((entry_width, key_count), queries.dtype),
            pltpu.VMEM((key_count, entry_width), queries.dtype),
            pltpu.VMEM((key_count, token_count), jnp.float32),
        ],
    )


def layer(
    queries, latents, block_starts, w_uv, moe_tokens, expert_ids, gate_weights, w_gate, w_up, w_down
):
    token_count, picks = expert_ids.shape
    expert_count = lax.axis_size("exp")
    ctx_size = lax.axis_size("ctx")
    width = moe_tokens.shape[1] // ctx_size
    capacity = 3 * token_count * picks // (2 * expert_count)
    where = where_am_i()
    evens = range(2, ctx_size, 2)

    slices = split_columns(w_down[0], width, where)
    down_parts = [swap(slices[offset - 1], "ctx", offset) for offset in range(1, ctx_size)]

    sets = set_members(expert_count)
    doubled = sets[-1] if is_doubled(ctx_size, width) else []
    outgoing = dispatch(
        moe_tokens, expert_ids.T, capacity, expert_count, width, doubled, where
    )
    arrived = [swap(outgoing[k], "exp", k) if k else outgoing[0] for k in range(expert_count)]

    returned = [None] * expert_count
    for members in sets:
        own = pack([arrived[k] for k in members], where)
        beside = swap(own, "ctx", 1)
        if own.shape[1] > width:
            early, late = [(own, 0, 0), (own, 1, 2)], [(beside, 0, 1), (beside, 1, 3)]
        else:
            early, late = [(own, 0, 0), (beside, 0, 1)], []
            for offset in evens:
                crossed = swap(own, "ctx", offset)
                late += [(crossed, 0, offset)]
                late += [(swap(crossed, "ctx", 1), 0, offset + 1)]
        partial = mlp(early, width, w_gate[0], w_up[0], None, where)
        hidden = mlp(late, width, w_gate[0], w_up[0], partial, where)
        hidden = [hidden] + [swap(hidden, "ctx", offset) for offset in range(1, ctx_size)]
        blocks = down(hidden, w_down[0], down_parts, len(members), where)
        for k, block in zip(members, blocks):
            returned[k] = swap(block, "exp", k) if k else block

    keys = [latents.T] + [None] * (ctx_size - 1)
    for offset in evens:
        keys[offset] = swap(keys[0], "ctx", offset)
    for offset in range(0, ctx_size, 2):
        keys[offset + 1] = swap(keys[offset], "ctx", 1)
    attended = attention(jnp.transpose(queries, (1, 2, 0)), keys, block_starts, w_uv, where)
    attended = jnp.transpose(attended, (1, 0, 2))
    return attended, combine(returned, [sets[0], sets[2], sets[1]], expert_ids.T, gate_weights.T, where)


def solution(mesh):
    in_specs = (
        P("ctx", "exp", None),
        P("ctx", None),
        P(),
        P("exp", None, None),
        P("exp", None),
        P("exp", None),
        P("exp", None),
        P("exp", None, "ctx"),
        P("exp", None, "ctx"),
        P("exp", "ctx", None),
    )
    out_specs = (P("ctx", "exp", None), P("exp", "ctx"))
    return jax.shard_map(layer, mesh=mesh, in_specs=in_specs, out_specs=out_specs, check_vma=False)
```
